512 devices in a mesh: edp: 32 (over z_hi, y, core), etp: 16 (over z_lo, x).
Axes of the slice: x: 4, y: 4, z: 16 (z_hi: 4, z_lo: 4; z = z_hi * 4 + z_lo), core: 2. Of those that a mesh axis runs over, the one named last changes fastest.
Arguments:
- tokens: bfloat16 [16384, 3072], P('edp'), may hold values from -6 to 6
- expert_ids: int32 [16384, 2], P('edp'), may hold values from 0 to 7, as said below
- route_weight: float32 [16384, 2], P('edp'), may hold values from 0.2 to 1
- index_list: int32 [32, 256], P('edp'), may hold values from 0 to 512, as said below
- gate_weight: bfloat16 [3072, 8192], P('edp', 'etp'), may hold values from -0.109375 to 0.109375
- up_weight: bfloat16 [3072, 8192], P('edp', 'etp'), may hold values from -0.109375 to 0.109375
- down_weight: bfloat16 [8192, 3072], P('etp', 'edp'), may hold values from -0.0625 to 0.0625
Outputs:
- expert_out: bfloat16 [16384, 3072], P(('edp', 'etp'))
The draws below stay inside these ranges and needn't reach their ends.
Inputs may be any that keep to these rules, and one draw needn't show every extreme that they name: `index_list`: row b lists, increasing, the positions within block b of the tokens that name expert 0, then 512 in the remaining slots; in every draw some block is full. `expert_ids`: each token names two different experts; a token names expert 0 exactly when its position stands in its block's row of index_list.
All inputs are finite; a program needn't handle non-finite values.
Results may differ from the reference program's by a relative error of at most 0.018.
Values may be sent and summed in bfloat16 or wider, within the bound.
No kernel may reach another device: no remote copies, remote signals or barrier semaphores. Data moves between devices by JAX's collectives and lax.ppermute only.
A program may use at most 64 MiB of HBM per device.

```python
import jax
import jax.numpy as jnp
from jax import lax

D = 3072
FF = 8192
NUM_EXPERTS = 8
TOK_DEV = 512
CAP = 256
BLOCKS = 32
TOKENS = 16384
N_ETP = 16


def routing(key):
    base_key = jax.random.fold_in(key, 7)
    k_shift, k_pick, k_perm, k_first, k_offset, k_order = jax.random.split(base_key, 6)
    halvings = jax.random.randint(k_shift, (BLOCKS,), 0, 4)
    counts = jnp.maximum(CAP // jnp.left_shift(jnp.ones_like(halvings), halvings), 1)
    full_block = jax.random.randint(k_pick, (), 0, BLOCKS)
    counts = jnp.where(jnp.arange(BLOCKS) == full_block, CAP, counts)
    perm_keys = jax.random.split(k_perm, BLOCKS)

    def permute(one_key):
        return jax.random.permutation(one_key, TOK_DEV)
    orders = jax.vmap(permute)(perm_keys)
    ranking = jnp.argsort(orders, axis=1)
    chosen = ranking < counts[:, None]
    position = jnp.arange(TOK_DEV)[None, :]
    scores = jnp.where(chosen, position, TOK_DEV + position)
    ordered = jnp.sort(scores, axis=1)[:, :CAP]
    index_list = jnp.where(ordered < TOK_DEV, ordered, TOK_DEV).astype(jnp.int32)
    first_pick = jax.random.randint(k_first, (BLOCKS, TOK_DEV), 1, NUM_EXPERTS)
    offsets = jax.random.randint(k_offset, (BLOCKS, TOK_DEV), 1, NUM_EXPERTS - 1)
    second_pick = 1 + (first_pick - 1 + offsets) % (NUM_EXPERTS - 1)
    leading = jnp.where(chosen, 0, first_pick)
    trailing = jnp.where(chosen, first_pick, second_pick)
    order_bit = jax.random.randint(k_order, (BLOCKS, TOK_DEV), 0, 2)
    left_ids = jnp.where(order_bit == 0, leading, trailing)
    right_ids = jnp.where(order_bit == 0, trailing, leading)
    expert_ids = jnp.stack([left_ids, right_ids], axis=-1).reshape(BLOCKS * TOK_DEV, 2).astype(jnp.int32)
    return (expert_ids, index_list)


def draw_expert_ids(key, part):
    return routing(key)[0]


def draw_index_list(key, part):
    return routing(key)[1]


def block_scale(rng, shape, cuts, smallest, top_value):
    factor_of = 1.0
    for dim, blocks in cuts:
        draws = jax.random.uniform(jax.random.fold_in(jax.random.fold_in(rng, 6), dim), (blocks,), jnp.float32, smallest / len(cuts), top_value / len(cuts))
        factor_of = factor_of * jnp.repeat(jnp.exp(draws), shape[dim] // blocks).reshape((-1,) + (1,) * (len(shape) - 1 - dim))
    return factor_of


def noise(rng, extent, scale, limit, shards=(), held_as=jnp.bfloat16):
    entries = jax.random.normal(rng, extent, jnp.float32) * scale
    if len(shards) > 0:
        entries = block_scale(rng, extent, shards, -0.22, 0.18) * entries
    return jnp.clip(entries, min=-limit, max=limit).astype(held_as)


def setup_inputs(seed: int = 0) -> dict:
    key_list = jax.random.split(jax.random.key(seed), 8)
    tokens = noise(key_list[0], (TOKENS, D), 1.0, 6.0, ((0, 32),))
    expert_ids = draw_expert_ids(jax.random.fold_in(key_list[7], 71), 0)
    route_weight = jnp.clip(0.2 + 0.8 * jax.random.uniform(key_list[2], (TOKENS, 2), jnp.float32) ** block_scale(key_list[2], (TOKENS, 2), ((0, 32),), -0.2, 0.2), 0.2, 1.0)
    index_list = draw_index_list(jax.random.fold_in(key_list[7], 71), 0)
    gate_weight = noise(key_list[4], (D, FF), D ** -0.5, 0.109375, ((0, 32), (1, 16)))
    up_weight = noise(key_list[5], (D, FF), D ** -0.5, 0.109375, ((0, 32), (1, 16)))
    down_weight = noise(key_list[6], (FF, D), FF ** -0.5, 0.0625, ((0, 16), (1, 32)))
    return dict(tokens=tokens, expert_ids=expert_ids, route_weight=route_weight, index_list=index_list, gate_weight=gate_weight, up_weight=up_weight, down_weight=down_weight)


def reference(tokens, expert_ids, route_weight, index_list, gate_weight, up_weight, down_weight):
    block_count = index_list.shape[0]
    block_rows = tokens.shape[0] // block_count
    combine = jnp.sum(jnp.where(expert_ids == 0, route_weight, jnp.zeros_like(route_weight)), axis=1)
    width = FF // N_ETP
    down_parts = down_weight.reshape(N_ETP, width, D).astype(jnp.float32)

    def one_block(block_index):
        row_start = (block_index * block_rows).astype(jnp.int32)
        local_rows = lax.dynamic_slice_in_dim(tokens, row_start, block_rows, 0)
        local_combine = lax.dynamic_slice_in_dim(combine, row_start, block_rows, 0)
        slot_rows = index_list[block_index].astype(jnp.int32)
        is_live = slot_rows < block_rows
        safe_rows = jnp.minimum(slot_rows, block_rows - 1).astype(jnp.int32)
        picked = jnp.take(local_rows, safe_rows, axis=0)
        row_scale = jnp.where(is_live, jnp.take(local_combine, safe_rows), jnp.zeros_like(local_combine[:1]))
        gate_sum = jnp.dot(picked, gate_weight, preferred_element_type=jnp.float32)
        up_sum = jnp.dot(picked, up_weight, preferred_element_type=jnp.float32)
        hidden = (jax.nn.silu(gate_sum) * up_sum * row_scale[:, None]).astype(jnp.bfloat16)
        pieces = hidden.reshape(CAP, N_ETP, width).astype(jnp.float32)
        partial_terms = jnp.einsum("rkf,kfd->krd", pieces, down_parts)
        rounded = lax.optimization_barrier(partial_terms.astype(jnp.bfloat16))
        shares = jnp.sum(rounded.astype(jnp.float32), axis=0).astype(jnp.bfloat16)
        empty = jnp.zeros((block_rows, D), jnp.bfloat16)
        return empty.at[slot_rows].set(shares, mode="drop")

    result = lax.map(one_block, jnp.arange(block_count, dtype=jnp.int32))
    return result.reshape(block_count * block_rows, D)
```

```python
import functools
import jax
import jax.numpy as jnp
from jax import lax
from jax.experimental import pallas as pl
from jax.experimental.pallas import tpu as pltpu
from jax.sharding import Mesh, PartitionSpec as P


BF = jnp.bfloat16
F32 = jnp.float32
STREAMS = 1


def vm():
    return pl.BlockSpec(memory_space=pltpu.VMEM)


def sm():
    return pl.BlockSpec(memory_space=pltpu.SMEM)


def call(body, out, ins, name, scratch=(), flops=0, byts=0):
    return pl.pallas_call(
        body,
        out_shape=out,
        in_specs=ins,
        out_specs=vm(),
        scratch_shapes=scratch,
        name=name,
        cost_estimate=pl.CostEstimate(flops=flops, transcendentals=0, bytes_accessed=byts),
        compiler_params=pltpu.CompilerParams(vmem_limit_bytes=40 * 1024 * 1024),
    )


def dot_nn(a, b):
    return lax.dot_general(a, b, (((1,), (0,)), ((), ())), preferred_element_type=F32)


def dot_nt(a, b):
    return lax.dot_general(a, b, (((1,), (1,)), ((), ())), preferred_element_type=F32)


def pick_body(idx_ref, tok_ref, out_ref):
    caps, rows = idx_ref.shape[0], tok_ref.shape[0]
    hot = (lax.broadcasted_iota(jnp.int32, (caps, rows), 1) == idx_ref[...]).astype(BF)
    width = out_ref.shape[2]
    for m in range(out_ref.shape[0]):
        out_ref[m] = dot_nn(hot, tok_ref[:, m * width : (m + 1) * width]).astype(BF)


def hidden_body(ord_ref, own_ref, mate_ref, first_ref, second_ref, out_ref):
    caps, width = own_ref.shape[1], own_ref.shape[2]
    half = first_ref.shape[0] // width
    core = ord_ref[16]
    for src, place in ((own_ref, core), (mate_ref, 1 - core)):
        acc = None
        for k in range(2 * half):
            wref = first_ref if k < half else second_ref
            lo = (k % half) * width
            part = dot_nn(src[ord_ref[k]], wref[lo : lo + width, :])
            acc = part if acc is None else acc + part
        cols = []
        for s in range(acc.shape[1] // 256):
            gate = acc[:, 256 * s : 256 * s + 128]
            up = acc[:, 256 * s + 128 : 256 * s + 256]
            cols.append((gate / (1.0 + jnp.exp(-gate)) * up).astype(BF))
        res = cols[0] if len(cols) == 1 else jnp.concatenate(cols, axis=1)
        out_ref[pl.ds(pl.multiple_of(place * caps, caps), caps), :] = res


def down_body(ord_ref, idx_ref, first_ref, second_ref, *rest):
    hid_refs, out_ref, scr = rest[:-2], rest[-2], rest[-1]
    caps = idx_ref.shape[1]
    rows = 512
    unit = 24
    groups = hid_refs[0].shape[0]
    for n, wref in enumerate((first_ref, second_ref)):
        acc = None
        for g in range(groups):
            core, x = g // 4, g % 4
            hid = [h[g] for h in hid_refs]
            hid = hid[0] if len(hid) == 1 else jnp.concatenate(hid, axis=1)
            lo = 512 * x + 256 * core
            part = dot_nt(wref[:, lo : lo + 256], hid)
            acc = part if acc is None else acc + part
        half = wref.shape[0] // unit
        for k in range(half):
            m = ord_ref[n * half + k]
            scr[pl.ds(pl.multiple_of(m * unit, 8), unit), :] = acc[k * unit : (k + 1) * unit, :]
    for b in range(2):
        hot = (lax.broadcasted_iota(jnp.int32, (rows, caps), 0) == idx_ref[b : b + 1, :]).astype(BF)
        dense = dot_nt(scr[:, b * caps : (b + 1) * caps].astype(BF), hot).astype(BF)
        for q in range(4):
            out_ref[q, :, b * 128 : (b + 1) * 128] = dense[:, q * 128 : (q + 1) * 128]


def total_body(in_ref, out_ref):
    acc = in_ref[0].astype(F32)
    for q in range(1, 4):
        acc = acc + in_ref[q].astype(F32)
    out_ref[...] = acc.T.astype(BF)


def place_body(in_ref, scale_ref, out_ref, scr):
    unit = 24
    for g in range(8):
        turned = in_ref[g].astype(F32).T
        core, x = g // 4, g % 4
        for m in range(16):
            lo = 192 * m + 96 * core + unit * x
            scr[lo : lo + unit, :] = turned[m * unit : (m + 1) * unit, :]
    for n in range(6):
        out_ref[:, n * 512 : (n + 1) * 512] = (scr[n * 512 : (n + 1) * 512, :].T * scale_ref[...]).astype(BF)


def pairs(step):
    flips = ((1, 3), (3, 1))
    return [(2 * i + c, 2 * (i ^ flips[c][step]) + c) for i in range(4) for c in range(2)]


def meet(value, axis, step):
    return lax.ppermute(value, (axis, "c"), pairs(step))


def gather_pair(value, axis):
    near = meet(value, axis, 0)
    both = jnp.concatenate([value, near], axis=0)
    return both, meet(both, axis, 1)


def gather16(value):
    both, far = gather_pair(value, "zh")
    return gather_pair(jnp.concatenate([both, far], axis=0), "y")


def shards(tokens, expert_ids, route_weight, index_list, gate_weight, up_weight, down_weight):
    zh, y, c, zl, x = (lax.axis_index(n) for n in ("zh", "y", "c", "zl", "x"))
    caps = index_list.shape[1]

    cut = lambda w, n: w[:, 128 * n : 128 * n + 128]
    mine = [
        jnp.concatenate([cut(w, 2 * h + s) for s in range(2) for w in (gate_weight, up_weight)], axis=1)
        for h in range(2)
    ]
    both_rows = lax.all_to_all(jnp.concatenate(mine, axis=0), "c", 0, 0, tiled=True)

    turned = down_weight.T
    quarter = lax.all_to_all(turned, "x", 0, 0, tiled=True)
    quarter = quarter.reshape(4, 24, 512).transpose(1, 0, 2).reshape(24, 2048)

    flip = jnp.where(c == 0, jnp.array([0, 1, 3, 2]), jnp.array([0, 3, 1, 2])).astype(jnp.int32)
    order = ((zh ^ flip)[None, :] * 4 + (y ^ flip)[:, None]).reshape(16)
    order = jnp.concatenate([order, c.reshape(1)]).astype(jnp.int32)

    rows = call(
        pick_body, jax.ShapeDtypeStruct((16, caps, 192), BF), [vm(), vm()], "pick", flops=2 * 256 * 512 * 3072
    )(index_list.reshape(caps, 1), tokens)
    swap = [(0, 1), (1, 0)]
    rows_mate = lax.ppermute(rows, "c", swap)
    index_mate = lax.ppermute(index_list, "c", swap)
    index_both = jnp.where(
        c == 0,
        jnp.concatenate([index_list, index_mate], axis=0),
        jnp.concatenate([index_mate, index_list], axis=0),
    )

    width = 512 // STREAMS
    ups = [gather16(both_rows[:, n * width : (n + 1) * width]) for n in range(STREAMS)]
    down_first, down_second = gather16(quarter)

    hids = []
    for first, second in ups:
        h = call(
            hidden_body,
            jax.ShapeDtypeStruct((2 * caps, width // 2), BF),
            [sm(), vm(), vm(), vm(), vm()],
            "hidden",
            flops=2 * 512 * 3072 * width,
        )(order, rows, rows_mate, first, second)
        wide = jnp.broadcast_to(h[None], (8,) + h.shape)
        hids.append(lax.all_to_all(wide, ("c", "x"), 0, 0, tiled=True))

    parts = call(
        down_body,
        jax.ShapeDtypeStruct((4, 384, 256), BF),
        [sm(), vm(), vm(), vm()] + [vm()] * len(hids),
        "down",
        scratch=[pltpu.VMEM((384, 512), F32)],
        flops=2 * 512 * 384 * 2048,
    )(order, index_both, down_first, down_second, *hids)
    parts = lax.all_to_all(parts, "zl", 0, 0, tiled=True)
    total = call(total_body, jax.ShapeDtypeStruct((256, 384), BF), [vm()], "total")(parts)
    owned = lax.all_to_all(total.reshape(8, 32, 384), ("c", "x"), 0, 0, tiled=True)

    start = (zl * 4 + x) * 32
    ids = lax.dynamic_slice_in_dim(expert_ids, start, 32, 0)
    weights = lax.dynamic_slice_in_dim(route_weight, start, 32, 0)
    scale = jnp.sum(jnp.where(ids == 0, weights, jnp.zeros_like(weights)), axis=1, keepdims=True)
    return call(
        place_body,
        jax.ShapeDtypeStruct((32, 3072), BF),
        [vm(), vm()],
        "place",
        scratch=[pltpu.VMEM((3072, 32), F32)],
    )(owned, scale)


def solution(mesh):
    fine = Mesh(mesh.devices.reshape(4, 4, 2, 4, 4), ("zh", "y", "c", "zl", "x"))
    edp, etp = ("zh", "y", "c"), ("zl", "x")
    in_specs = (P(edp, None), P(edp, None), P(edp, None), P(edp, None), P(edp, etp), P(edp, etp), P(etp, edp))
    return jax.shard_map(
        shards, mesh=fine, in_specs=in_specs, out_specs=P(edp + etp, None), check_vma=False
    )
```

```python
import jax
import jax.numpy as jnp
from jax import lax
from jax.experimental import pallas as pl
from jax.experimental.pallas import tpu as pltpu
from jax.sharding import Mesh, PartitionSpec as P


BF = jnp.bfloat16
F32 = jnp.float32
STREAMS = 2


def vm():
    return pl.BlockSpec(memory_space=pltpu.VMEM)


def sm():
    return pl.BlockSpec(memory_space=pltpu.SMEM)


def call(body, out, ins, scratch=(), flops=0, byts=0):
    return pl.pallas_call(
        body,
        out_shape=out,
        in_specs=ins,
        out_specs=vm(),
        scratch_shapes=scratch,
        cost_estimate=pl.CostEstimate(flops=flops, transcendentals=0, bytes_accessed=byts),
        compiler_params=pltpu.CompilerParams(vmem_limit_bytes=40 * 1024 * 1024),
    )


def dot_nn(a, b):
    return lax.dot_general(a, b, (((1,), (0,)), ((), ())), preferred_element_type=F32)


def dot_nt(a, b):
    return lax.dot_general(a, b, (((1,), (1,)), ((), ())), preferred_element_type=F32)


def pick_body(idx_ref, tok_ref, out_ref):
    caps, rows = idx_ref.shape[0], tok_ref.shape[0]
    hot = (lax.broadcasted_iota(jnp.int32, (caps, rows), 1) == idx_ref[...]).astype(BF)
    width = tok_ref.shape[1] // out_ref.shape[0]
    pad = jnp.zeros((caps, out_ref.shape[2] - width), BF)
    for m in range(out_ref.shape[0]):
        out_ref[m, :, :width] = dot_nn(hot, tok_ref[:, m * width : (m + 1) * width]).astype(BF)
        out_ref[m, :, width:] = pad


def hidden_body(ord_ref, own_ref, mate_ref, first_ref, second_ref, out_ref):
    caps, width = own_ref.shape[1], 192
    half = first_ref.shape[0] // width
    core = ord_ref[16]
    for src, place in ((own_ref, core), (mate_ref, 1 - core)):
        acc = None
        for k in range(2 * half):
            wref = first_ref if k < half else second_ref
            lo = (k % half) * width
            part = dot_nn(src[ord_ref[k], :, :width], wref[lo : lo + width, :])
            acc = part if acc is None else acc + part
        cols = []
        for s in range(acc.shape[1] // 256):
            gate = acc[:, 256 * s : 256 * s + 128]
            up = acc[:, 256 * s + 128 : 256 * s + 256]
            cols.append((gate / (1.0 + jnp.exp(-gate)) * up).astype(BF))
        res = cols[0] if len(cols) == 1 else jnp.concatenate(cols, axis=1)
        out_ref[pl.ds(pl.multiple_of(place * caps, caps), caps), :] = res


def down_body(ord_ref, idx_ref, first_ref, second_ref, *rest):
    hid_refs, out_ref, scr = rest[:-2], rest[-2], rest[-1]
    caps = idx_ref.shape[1]
    rows = 512
    unit = 24
    groups = hid_refs[0].shape[0]
    for n, wref in enumerate((first_ref, second_ref)):
        acc = None
        for g in range(groups):
            core, x = g // 4, g % 4
            hid = [h[g] for h in hid_refs]
            hid = hid[0] if len(hid) == 1 else jnp.concatenate(hid, axis=1)
            lo = 512 * x + 256 * core
            part = dot_nt(wref[:, lo : lo + 256], hid)
            acc = part if acc is None else acc + part
        half = wref.shape[0] // unit
        for k in range(half):
            m = ord_ref[n * half + k]
            scr[pl.ds(pl.multiple_of(m * unit, 8), unit), :] = acc[k * unit : (k + 1) * unit, :]
    for b in range(2):
        hot = (lax.broadcasted_iota(jnp.int32, (rows, caps), 0) == idx_ref[b : b + 1, :]).astype(BF)
        dense = dot_nt(scr[:, b * caps : (b + 1) * caps].astype(BF), hot).astype(BF)
        for q in range(4):
            out_ref[q, :, b * 128 : (b + 1) * 128] = dense[:, q * 128 : (q + 1) * 128]


def quarter_body(in_ref, out_ref):
    for x in range(4):
        out_ref[:, 512 * x : 512 * (x + 1)] = in_ref[24 * x : 24 * (x + 1), :]


def total_body(in_ref, out_ref):
    acc = in_ref[0].astype(F32)
    for q in range(1, 4):
        acc = acc + in_ref[q].astype(F32)
    out_ref[...] = acc.T.astype(BF)


def place_body(in_ref, scale_ref, out_ref, scr):
    unit = 24
    for g in range(8):
        turned = in_ref[g].astype(F32).T
        core, x = g // 4, g % 4
        for m in range(16):
            lo = 192 * m + 96 * core + unit * x
            scr[lo : lo + unit, :] = turned[m * unit : (m + 1) * unit, :]
    for n in range(6):
        out_ref[:, n * 512 : (n + 1) * 512] = (scr[n * 512 : (n + 1) * 512, :].T * scale_ref[...]).astype(BF)


def pairs(step):
    flips = ((1, 3), (3, 1))
    return [(2 * i + c, 2 * (i ^ flips[c][step]) + c) for i in range(4) for c in range(2)]


def join_body(a_ref, b_ref, out_ref):
    rows = a_ref.shape[0]
    out_ref[:rows, :] = a_ref[...]
    out_ref[rows:, :] = b_ref[...]


def join(a, b):
    out = jax.ShapeDtypeStruct((a.shape[0] + b.shape[0], a.shape[1]), BF)
    return call(join_body, out, [vm(), vm()])(a, b)


def meet(value, axis, step):
    return lax.ppermute(value, (axis, "c"), pairs(step))


def gather16(value):
    near = meet(value, "zh", 0)
    both = join(value, near)
    far = meet(both, "zh", 1)
    four = join(both, far)
    near = meet(four, "y", 0)
    both = join(four, near)
    return both, meet(both, "y", 1)


def shards(tokens, expert_ids, route_weight, index_list, gate_weight, up_weight, down_weight):
    zh, y, c, zl, x = (lax.axis_index(n) for n in ("zh", "y", "c", "zl", "x"))
    caps = index_list.shape[1]

    cut = lambda w, n: w[:, 128 * n : 128 * n + 128]
    mine = [
        jnp.concatenate([cut(w, 2 * h + s) for s in range(2) for w in (gate_weight, up_weight)], axis=1)
        for h in range(2)
    ]
    both_rows = lax.all_to_all(jnp.concatenate(mine, axis=0), "c", 0, 0, tiled=True)

    turned = down_weight.T
    quarter = lax.all_to_all(turned, "x", 0, 0, tiled=True)
    quarter = call(quarter_body, jax.ShapeDtypeStruct((24, 2048), BF), [vm()])(quarter)

    flip = jnp.where(c == 0, jnp.array([0, 1, 3, 2]), jnp.array([0, 3, 1, 2])).astype(jnp.int32)
    order = ((zh ^ flip)[None, :] * 4 + (y ^ flip)[:, None]).reshape(16)
    order = jnp.concatenate([order, c.reshape(1)]).astype(jnp.int32)

    rows = call(
        pick_body, jax.ShapeDtypeStruct((16, caps, 256), BF), [vm(), vm()], flops=2 * 256 * 512 * 3072
    )(index_list.reshape(caps, 1), tokens)
    swap = [(0, 1), (1, 0)]
    rows_mate = lax.ppermute(rows, "c", swap)
    index_mate = lax.ppermute(index_list, "c", swap)
    index_both = jnp.where(
        c == 0,
        jnp.concatenate([index_list, index_mate], axis=0),
        jnp.concatenate([index_mate, index_list], axis=0),
    )

    width = 512 // STREAMS
    ups = [gather16(both_rows[:, n * width : (n + 1) * width]) for n in range(STREAMS)]
    down_first, down_second = gather16(quarter)

    hids = []
    for first, second in ups:
      h = call(
          hidden_body,
          jax.ShapeDtypeStruct((2 * caps, width // 2), BF),
          [sm(), vm(), vm(), vm(), vm()],
          flops=2 * 512 * 3072 * width,
      )(order, rows, rows_mate, first, second)
      wide = jnp.broadcast_to(h[None], (8,) + h.shape)
      hids.append(lax.all_to_all(wide, ("c", "x"), 0, 0, tiled=True))

    parts = call(
        down_body,
        jax.ShapeDtypeStruct((4, 384, 256), BF),
        [sm(), vm(), vm(), vm()] + [vm()] * len(hids),
        scratch=[pltpu.VMEM((384, 512), F32)],
        flops=2 * 512 * 384 * 2048,
    )(order, index_both, down_first, down_second, *hids)
    parts = lax.all_to_all(parts, "zl", 0, 0, tiled=True)
    total = call(total_body, jax.ShapeDtypeStruct((256, 384), BF), [vm()])(parts)
    owned = lax.all_to_all(total.reshape(8, 32, 384), ("c", "x"), 0, 0, tiled=True)

    start = (zl * 4 + x) * 32
    ids = lax.dynamic_slice_in_dim(expert_ids, start, 32, 0)
    weights = lax.dynamic_slice_in_dim(route_weight, start, 32, 0)
    scale = jnp.sum(jnp.where(ids == 0, weights, jnp.zeros_like(weights)), axis=1, keepdims=True)
    return call(
        place_body, jax.ShapeDtypeStruct((32, 3072), BF), [vm(), vm()], scratch=[pltpu.VMEM((3072, 32), F32)]
    )(owned, scale)


def solution(mesh):
    fine = Mesh(mesh.devices.reshape(4, 4, 2, 4, 4), ("zh", "y", "c", "zl", "x"))
    edp, etp = ("zh", "y", "c"), ("zl", "x")
    in_specs = (P(edp, None), P(edp, None), P(edp, None), P(edp, None), P(edp, etp), P(edp, etp), P(etp, edp))

    return jax.shard_map(shards, mesh=fine, in_specs=in_specs, out_specs=P(edp + etp, None), check_vma=False)
```

```python
import jax
import jax.numpy as jnp
from jax import lax
from jax.experimental import pallas as pl
from jax.experimental.pallas import tpu as pltpu
from jax.sharding import Mesh, PartitionSpec as P


BF = jnp.bfloat16
F32 = jnp.float32


def vm():
    return pl.BlockSpec(memory_space=pltpu.VMEM)


def sm():
    return pl.BlockSpec(memory_space=pltpu.SMEM)


def hb():
    return pl.BlockSpec(memory_space=pltpu.HBM)


def call(body, out, ins, scratch=(), flops=0, mib=16, to=vm):
    return pl.pallas_call(
        body,
        out_shape=out,
        in_specs=ins,
        out_specs=to(),
        scratch_shapes=scratch,
        cost_estimate=pl.CostEstimate(flops=flops, transcendentals=0, bytes_accessed=0),
        compiler_params=pltpu.CompilerParams(vmem_limit_bytes=mib * 1024 * 1024),
    )


def dot_nn(a, b):
    return lax.dot_general(a, b, (((1,), (0,)), ((), ())), preferred_element_type=F32)


def dot_nt(a, b):
    return lax.dot_general(a, b, (((1,), (1,)), ((), ())), preferred_element_type=F32)


def pick_body(idx_ref, tok_ref, out_ref):
    caps, rows = idx_ref.shape[0], tok_ref.shape[0]
    hot = (lax.broadcasted_iota(jnp.int32, (caps, rows), 1) == idx_ref[...]).astype(BF)
    width = tok_ref.shape[1] // out_ref.shape[0]
    pad = jnp.zeros((caps, out_ref.shape[2] - width), BF)
    for m in range(out_ref.shape[0]):
        out_ref[m, :, :width] = dot_nn(hot, tok_ref[:, m * width : (m + 1) * width]).astype(BF)
        out_ref[m, :, width:] = pad


def mix(ord_ref, src, wrefs, spots):
    width, acc = 192, None
    for wref, places in zip(wrefs, spots):
        pieces = len(places) // 4
        for n, k in enumerate(places):
            lo = (n % pieces) * width
            part = dot_nn(src[ord_ref[k], :, :width], wref[n // pieces, lo : lo + width, :])
            acc = part if acc is None else acc + part
    return acc


def early_body(ord_ref, own_ref, mate_ref, a_ref, b_ref, out_ref):
    caps = own_ref.shape[1]
    spots = ([4 * q for q in range(4)], [4 * q + 1 for q in range(4)])
    for n, src in enumerate((own_ref, mate_ref)):
        out_ref[n * caps : (n + 1) * caps, :] = mix(ord_ref, src, (a_ref, b_ref), spots)


def hidden_body(ord_ref, own_ref, mate_ref, early_ref, c_ref, out_ref, res_ref, sems):
    caps = own_ref.shape[1]
    core = ord_ref[32]
    spots = ([4 * q + n for q in range(4) for n in (2, 3)],)
    for n, src in enumerate((own_ref, mate_ref)):
        acc = early_ref[n * caps : (n + 1) * caps, :] + mix(ord_ref, src, (c_ref,), spots)
        cols = []
        for s in range(2):
            gate = acc[:, 256 * s : 256 * s + 128]
            up = acc[:, 256 * s + 128 : 256 * s + 256]
            cols.append((gate / (1.0 + jnp.exp(-gate)) * up).astype(BF))
        at = pl.multiple_of((core if n == 0 else 1 - core) * caps, caps)
        res_ref[pl.ds(at, caps), :] = jnp.concatenate(cols, axis=1)
    copies = [pltpu.make_async_copy(res_ref, out_ref.at[g], sems.at[g]) for g in range(8)]
    for copy in copies:
        copy.start()
    for copy in copies:
        copy.wait()


def down_body(ord_ref, idx_ref, first_ref, second_ref, hid_ref, out_ref, scr, second_vmem, sem):
    caps = idx_ref.shape[1]
    rows, unit = 512, 24
    fetch = pltpu.make_async_copy(second_ref, second_vmem, sem)
    fetch.start()
    for n, w_ref in enumerate((first_ref, second_vmem)):
        if n == 1:
            fetch.wait()
        acc = None
        for g in range(8):
            lo = 512 * (g % 4) + 256 * (g // 4)
            part = dot_nt(w_ref[:, lo : lo + 256], hid_ref[g])
            acc = part if acc is None else acc + part
        for k in range(8):
            at = pl.multiple_of(ord_ref[16 + 8 * n + k] * unit, 8)
            scr[pl.ds(at, unit), :] = acc[k * unit : (k + 1) * unit, :]
    for b in range(2):
        hot = (lax.broadcasted_iota(jnp.int32, (rows, caps), 0) == idx_ref[b : b + 1, :]).astype(BF)
        dense = dot_nt(scr[:, b * caps : (b + 1) * caps].astype(BF), hot).astype(BF)
        for q in range(4):
            out_ref[q, :, b * 128 : (b + 1) * 128] = dense[:, q * 128 : (q + 1) * 128]


def spread_body(*refs):
    out_ref, sems = refs[-2], refs[-1]
    lo, copies = 0, []
    for n, r in enumerate(refs[:-2]):
        for q in range(out_ref.shape[0]):
            copies.append(pltpu.make_async_copy(r, out_ref.at[q, pl.ds(lo, r.shape[0])], sems.at[n, q]))
        lo += r.shape[0]
    for copy in copies:
        copy.start()
    for copy in copies:
        copy.wait()


def quarter_body(in_ref, out_ref):
    for x in range(4):
        out_ref[:, 512 * x : 512 * (x + 1)] = in_ref[24 * x : 24 * (x + 1), :]


def total_body(in_ref, out_ref):
    acc = in_ref[0].astype(F32)
    for q in range(1, 4):
        acc = acc + in_ref[q].astype(F32)
    out_ref[...] = acc.T.astype(BF)


def place_body(in_ref, scale_ref, out_ref, scr):
    unit = 24
    for g in range(8):
        turned = in_ref[g].astype(F32).T
        core, x = g // 4, g % 4
        for m in range(16):
            lo = 192 * m + 96 * core + unit * x
            scr[lo : lo + unit, :] = turned[m * unit : (m + 1) * unit, :]
    for n in range(6):
        out_ref[:, n * 512 : (n + 1) * 512] = (scr[n * 512 : (n + 1) * 512, :].T * scale_ref[...]).astype(BF)


def pairs(step):
    flips = ((1, 3), (3, 1))
    return [(2 * i + c, 2 * (i ^ flips[c][step]) + c) for i in range(4) for c in range(2)]


def join_body(a_ref, b_ref, out_ref):
    rows = a_ref.shape[0]
    out_ref[:rows, :] = a_ref[...]
    out_ref[rows:, :] = b_ref[...]


def join(a, b):
    out = jax.ShapeDtypeStruct((a.shape[0] + b.shape[0], a.shape[1]), BF)
    return call(join_body, out, [vm(), vm()], mib=4)(a, b)


def meet(value, axis, step):
    return lax.ppermute(value, (axis, "c"), pairs(step))


def over_y(parts):
    rows, cols = sum(p.shape[0] for p in parts), parts[0].shape[1]
    wide = call(
        spread_body,
        jax.ShapeDtypeStruct((4, rows, cols), BF),
        [vm()] * len(parts),
        scratch=[pltpu.SemaphoreType.DMA((len(parts), 4))],
        mib=4,
        to=hb,
    )(*parts)
    return lax.all_to_all(wide, "y", 0, 0, tiled=True)


def shards(tokens, expert_ids, route_weight, index_list, gate_weight, up_weight, down_weight):
    zh, y, c, zl, x = (lax.axis_index(n) for n in ("zh", "y", "c", "zl", "x"))
    caps = index_list.shape[1]

    cut = lambda w, n: w[:, 128 * n : 128 * n + 128]
    mine = [
        jnp.concatenate([cut(w, 2 * h + s) for s in range(2) for w in (gate_weight, up_weight)], axis=1)
        for h in range(2)
    ]
    both_rows = lax.all_to_all(jnp.concatenate(mine, axis=0), "c", 0, 0, tiled=True)

    turned = down_weight.T
    quarter = lax.all_to_all(turned, "x", 0, 0, tiled=True)
    quarter = call(quarter_body, jax.ShapeDtypeStruct((24, 2048), BF), [vm()], mib=4)(quarter)

    flip = jnp.where(c == 0, jnp.array([0, 1, 3, 2]), jnp.array([0, 3, 1, 2])).astype(jnp.int32)
    order = ((zh ^ flip)[None, :] * 4 + jnp.arange(4, dtype=jnp.int32)[:, None]).reshape(16)
    order_down = ((zh ^ flip)[None, :] * 4 + (y ^ flip)[:, None]).reshape(16)
    order = jnp.concatenate([order, order_down, c.reshape(1)]).astype(jnp.int32)

    rows = call(
        pick_body, jax.ShapeDtypeStruct((16, caps, 256), BF), [vm(), vm()], flops=2 * 256 * 512 * 3072
    )(index_list.reshape(caps, 1), tokens)
    swap = [(0, 1), (1, 0)]
    rows_mate = lax.ppermute(rows, "c", swap)
    index_mate = lax.ppermute(index_list, "c", swap)
    index_both = jnp.where(
        c == 0,
        jnp.concatenate([index_list, index_mate], axis=0),
        jnp.concatenate([index_mate, index_list], axis=0),
    )

    near = meet(both_rows, "zh", 0)
    far = meet(join(both_rows, near), "zh", 1)
    ya = over_y((both_rows,))
    yb = over_y((near,))
    yc = over_y((far,))

    near = meet(quarter, "zh", 0)
    two = join(quarter, near)
    far = meet(two, "zh", 1)
    four = join(two, far)
    near = meet(four, "y", 0)
    down_first = join(four, near)
    down_second = meet(down_first, "y", 1)

    early = call(
        early_body, jax.ShapeDtypeStruct((512, 512), F32), [sm()] + [vm()] * 4, flops=512 * 3072 * 512
    )(order, rows, rows_mate, ya, yb)
    wide = call(
        hidden_body, jax.ShapeDtypeStruct((8, 512, 256), BF), [sm()] + [vm()] * 4, flops=512 * 3072 * 512,
        scratch=[pltpu.VMEM((512, 256), BF), pltpu.SemaphoreType.DMA((8,))], to=hb,
    )(order, rows, rows_mate, early, yc)
    hid = lax.all_to_all(wide, ("c", "x"), 0, 0, tiled=True)

    parts = call(
        down_body,
        jax.ShapeDtypeStruct((4, 384, 256), BF),
        [sm(), vm(), vm(), hb(), vm()],
        scratch=[pltpu.VMEM((384, 512), F32), pltpu.VMEM((192, 2048), BF), pltpu.SemaphoreType.DMA],
        flops=2 * 512 * 384 * 2048,
    )(order, index_both, down_first, down_second, hid)
    parts = lax.all_to_all(parts, "zl", 0, 0, tiled=True)
    total = call(total_body, jax.ShapeDtypeStruct((256, 384), BF), [vm()], mib=8)(parts)
    owned = lax.all_to_all(total.reshape(8, 32, 384), ("c", "x"), 0, 0, tiled=True)

    start = (zl * 4 + x) * 32
    ids = lax.dynamic_slice_in_dim(expert_ids, start, 32, 0)
    weights = lax.dynamic_slice_in_dim(route_weight, start, 32, 0)
    scale = jnp.sum(jnp.where(ids == 0, weights, jnp.zeros_like(weights)), axis=1, keepdims=True)
    return call(
        place_body, jax.ShapeDtypeStruct((32, 3072), BF), [vm(), vm()], mib=8, scratch=[pltpu.VMEM((3072, 32), F32)]
    )(owned, scale)


def solution(mesh):
    fine = Mesh(mesh.devices.reshape(4, 4, 2, 4, 4), ("zh", "y", "c", "zl", "x"))
    edp, etp = ("zh", "y", "c"), ("zl", "x")
    in_specs = (P(edp, None), P(edp, None), P(edp, None), P(edp, None), P(edp, etp), P(edp, etp), P(etp, edp))

    return jax.shard_map(shards, mesh=fine, in_specs=in_specs, out_specs=P(edp + etp, None), check_vma=False)
```

```python
import jax
import jax.numpy as jnp
from jax import lax
from jax.experimental import pallas as pl
from jax.experimental.pallas import tpu as pltpu
from jax.sharding import Mesh, PartitionSpec as P


BF = jnp.bfloat16
F32 = jnp.float32


def vm():
    return pl.BlockSpec(memory_space=pltpu.VMEM)


def sm():
    return pl.BlockSpec(memory_space=pltpu.SMEM)


def hb():
    return pl.BlockSpec(memory_space=pltpu.HBM)


def call(body, out, ins, scratch=(), flops=0, mib=16, to=vm):
    return pl.pallas_call(
        body,
        out_shape=out,
        in_specs=ins,
        out_specs=to(),
        scratch_shapes=scratch,
        cost_estimate=pl.CostEstimate(flops=flops, transcendentals=0, bytes_accessed=0),
        compiler_params=pltpu.CompilerParams(vmem_limit_bytes=mib * 1024 * 1024),
    )


def dot_nn(a, b):
    return lax.dot_general(a, b, (((1,), (0,)), ((), ())), preferred_element_type=F32)


def dot_nt(a, b):
    return lax.dot_general(a, b, (((1,), (1,)), ((), ())), preferred_element_type=F32)


def pick_body(idx_ref, tok_ref, out_ref):
    caps, rows = idx_ref.shape[0], tok_ref.shape[0]
    hot = (lax.broadcasted_iota(jnp.int32, (caps, rows), 1) == idx_ref[...]).astype(BF)
    width = tok_ref.shape[1] // out_ref.shape[0]
    pad = jnp.zeros((caps, out_ref.shape[2] - width), BF)
    for m in range(out_ref.shape[0]):
        out_ref[m, :, :width] = dot_nn(hot, tok_ref[:, m * width : (m + 1) * width]).astype(BF)
        out_ref[m, :, width:] = pad


def mix(ord_ref, src, wrefs, spots):
    width, acc = 192, None
    for wref, places in zip(wrefs, spots):
        pieces = len(places) // 4
        for n, k in enumerate(places):
            lo = (n % pieces) * width
            part = dot_nn(src[ord_ref[k], :, :width], wref[n // pieces, lo : lo + width, :])
            acc = part if acc is None else acc + part
    return acc


def early_body(ord_ref, own_ref, mate_ref, ab_ref, out_ref):
    caps = own_ref.shape[1]
    spots = ([4 * q + n for q in range(4) for n in (0, 1)],)
    for n, src in enumerate((own_ref, mate_ref)):
        out_ref[n * caps : (n + 1) * caps, :] = mix(ord_ref, src, (ab_ref,), spots)


def hidden_body(ord_ref, own_ref, mate_ref, early_ref, c_ref, out_ref, res_ref, sems):
    caps = own_ref.shape[1]
    core = ord_ref[32]
    spots = ([4 * q + n for q in range(4) for n in (2, 3)],)
    for n, src in enumerate((own_ref, mate_ref)):
        acc = early_ref[n * caps : (n + 1) * caps, :] + mix(ord_ref, src, (c_ref,), spots)
        cols = []
        for s in range(2):
            gate = acc[:, 256 * s : 256 * s + 128]
            up = acc[:, 256 * s + 128 : 256 * s + 256]
            cols.append((gate / (1.0 + jnp.exp(-gate)) * up).astype(BF))
        at = pl.multiple_of((core if n == 0 else 1 - core) * caps, caps)
        res_ref[pl.ds(at, caps), :] = jnp.concatenate(cols, axis=1)
    copies = [pltpu.make_async_copy(res_ref, out_ref.at[g], sems.at[g]) for g in range(8)]
    for copy in copies:
        copy.start()
    for copy in copies:
        copy.wait()


def down_body(ord_ref, idx_ref, first_ref, second_ref, hid_ref, out_ref, scr, second_vmem, sem):
    caps = idx_ref.shape[1]
    rows, unit = 512, 24
    fetch = pltpu.make_async_copy(second_ref, second_vmem, sem)
    fetch.start()
    for n, w_ref in enumerate((first_ref, second_vmem)):
        if n == 1:
            fetch.wait()
        acc = None
        for g in range(8):
            lo = 512 * (g % 4) + 256 * (g // 4)
            part = dot_nt(w_ref[:, lo : lo + 256], hid_ref[g])
            acc = part if acc is None else acc + part
        for k in range(8):
            at = pl.multiple_of(ord_ref[16 + 8 * n + k] * unit, 8)
            scr[pl.ds(at, unit), :] = acc[k * unit : (k + 1) * unit, :]
    for b in range(2):
        hot = (lax.broadcasted_iota(jnp.int32, (rows, caps), 0) == idx_ref[b : b + 1, :]).astype(BF)
        dense = dot_nt(hot, scr[:, b * caps : (b + 1) * caps].astype(BF)).astype(BF)
        for n in range(16):
            out_ref[16 * b + n] = dense[32 * n : 32 * n + 32, :]


def spread_body(*refs):
    out_ref, sems = refs[-2], refs[-1]
    lo, copies = 0, []
    for n, r in enumerate(refs[:-2]):
        for q in range(out_ref.shape[0]):
            copies.append(pltpu.make_async_copy(r, out_ref.at[q, pl.ds(lo, r.shape[0])], sems.at[n, q]))
        lo += r.shape[0]
    for copy in copies:
        copy.start()
    for copy in copies:
        copy.wait()


def quarter_body(in_ref, out_ref):
    for x in range(4):
        out_ref[:, 512 * x : 512 * (x + 1)] = in_ref[24 * x : 24 * (x + 1), :]


def place_body(in_ref, scale_ref, out_ref, scr):
    unit = 24
    for g in range(8):
        core, x = g // 4, g % 4
        acc = in_ref[16 * core + x].astype(F32)
        for q in range(1, 4):
            acc = acc + in_ref[16 * core + 4 * q + x].astype(F32)
        turned = acc.T
        for m in range(16):
            lo = 192 * m + 96 * core + unit * x
            scr[lo : lo + unit, :] = turned[m * unit : (m + 1) * unit, :]
    for n in range(6):
        out_ref[:, n * 512 : (n + 1) * 512] = (scr[n * 512 : (n + 1) * 512, :].T * scale_ref[...]).astype(BF)


def pairs(step):
    flips = ((1, 3), (3, 1))
    return [(2 * i + c, 2 * (i ^ flips[c][step]) + c) for i in range(4) for c in range(2)]


def join_body(a_ref, b_ref, out_ref):
    rows = a_ref.shape[0]
    out_ref[:rows, :] = a_ref[...]
    out_ref[rows:, :] = b_ref[...]


def join(a, b):
    out = jax.ShapeDtypeStruct((a.shape[0] + b.shape[0], a.shape[1]), BF)
    return call(join_body, out, [vm(), vm()], mib=4)(a, b)


def meet(value, axis, step):
    return lax.ppermute(value, (axis, "c"), pairs(step))


def over_y(parts):
    rows, cols = sum(p.shape[0] for p in parts), parts[0].shape[1]
    wide = call(
        spread_body,
        jax.ShapeDtypeStruct((4, rows, cols), BF),
        [vm()] * len(parts),
        scratch=[pltpu.SemaphoreType.DMA((len(parts), 4))],
        mib=4,
        to=hb,
    )(*parts)
    return lax.all_to_all(wide, "y", 0, 0, tiled=True)


def shards(tokens, expert_ids, route_weight, index_list, gate_weight, up_weight, down_weight):
    zh, y, c, zl, x = (lax.axis_index(n) for n in ("zh", "y", "c", "zl", "x"))
    caps = index_list.shape[1]

    cut = lambda w, n: w[:, 128 * n : 128 * n + 128]
    mine = [
        jnp.concatenate([cut(w, 2 * h + s) for s in range(2) for w in (gate_weight, up_weight)], axis=1)
        for h in range(2)
    ]
    both_rows = lax.all_to_all(jnp.concatenate(mine, axis=0), "c", 0, 0, tiled=True)

    turned = down_weight.T
    quarter = lax.all_to_all(turned, "x", 0, 0, tiled=True)
    quarter = call(quarter_body, jax.ShapeDtypeStruct((24, 2048), BF), [vm()], mib=4)(quarter)

    flip = jnp.where(c == 0, jnp.array([0, 1, 3, 2]), jnp.array([0, 3, 1, 2])).astype(jnp.int32)
    order = ((zh ^ flip)[None, :] * 4 + jnp.arange(4, dtype=jnp.int32)[:, None]).reshape(16)
    order_down = ((zh ^ flip)[None, :] * 4 + (y ^ flip)[:, None]).reshape(16)
    order = jnp.concatenate([order, order_down, c.reshape(1)]).astype(jnp.int32)

    rows = call(
        pick_body, jax.ShapeDtypeStruct((16, caps, 256), BF), [vm(), vm()], flops=2 * 256 * 512 * 3072
    )(index_list.reshape(caps, 1), tokens)
    swap = [(0, 1), (1, 0)]
    rows_mate = lax.ppermute(rows, "c", swap)
    index_mate = lax.ppermute(index_list, "c", swap)
    index_both = jnp.where(
        c == 0,
        jnp.concatenate([index_list, index_mate], axis=0),
        jnp.concatenate([index_mate, index_list], axis=0),
    )

    near = meet(both_rows, "zh", 0)
    both = join(both_rows, near)
    far = meet(both, "zh", 1)
    yab = over_y((both,))
    yc = over_y((far,))

    near = meet(quarter, "zh", 0)
    two = join(quarter, near)
    far = meet(two, "zh", 1)
    four = join(two, far)
    near = meet(four, "y", 0)
    down_first = join(four, near)
    down_second = meet(down_first, "y", 1)

    early = call(
        early_body, jax.ShapeDtypeStruct((512, 512), F32), [sm()] + [vm()] * 3, flops=512 * 3072 * 512
    )(order, rows, rows_mate, yab)
    wide = call(
        hidden_body, jax.ShapeDtypeStruct((8, 512, 256), BF), [sm()] + [vm()] * 4, flops=512 * 3072 * 512,
        scratch=[pltpu.VMEM((512, 256), BF), pltpu.SemaphoreType.DMA((8,))], to=hb,
    )(order, rows, rows_mate, early, yc)
    hid = lax.all_to_all(wide, ("c", "x"), 0, 0, tiled=True)

    parts = call(
        down_body,
        jax.ShapeDtypeStruct((32, 32, 384), BF),
        [sm(), vm(), vm(), hb(), vm()],
        scratch=[pltpu.VMEM((384, 512), F32), pltpu.VMEM((192, 2048), BF), pltpu.SemaphoreType.DMA],
        flops=2 * 512 * 384 * 2048,
    )(order, index_both, down_first, down_second, hid)
    owned = lax.all_to_all(parts, ("c", "zl", "x"), 0, 0, tiled=True)

    start = (zl * 4 + x) * 32
    ids = lax.dynamic_slice_in_dim(expert_ids, start, 32, 0)
    weights = lax.dynamic_slice_in_dim(route_weight, start, 32, 0)
    scale = jnp.sum(jnp.where(ids == 0, weights, jnp.zeros_like(weights)), axis=1, keepdims=True)
    return call(
        place_body, jax.ShapeDtypeStruct((32, 3072), BF), [vm(), vm()], mib=8, scratch=[pltpu.VMEM((3072, 32), F32)]
    )(owned, scale)


def solution(mesh):
    fine = Mesh(mesh.devices.reshape(4, 4, 2, 4, 4), ("zh", "y", "c", "zl", "x"))
    edp, etp = ("zh", "y", "c"), ("zl", "x")
    in_specs = (P(edp, None), P(edp, None), P(edp, None), P(edp, None), P(edp, etp), P(edp, etp), P(etp, edp))

    return jax.shard_map(shards, mesh=fine, in_specs=in_specs, out_specs=P(edp + etp, None), check_vma=False)
```

```python
import jax
import jax.numpy as jnp
from jax import lax
from jax.experimental import pallas as pl
from jax.experimental.pallas import tpu as pltpu
from jax.sharding import Mesh, PartitionSpec as P


BF = jnp.bfloat16
F32 = jnp.float32


def vm():
    return pl.BlockSpec(memory_space=pltpu.VMEM)


def sm():
    return pl.BlockSpec(memory_space=pltpu.SMEM)


def hb():
    return pl.BlockSpec(memory_space=pltpu.HBM)


def call(body, out, ins, scratch=(), flops=0, mib=16, to=vm):
    return pl.pallas_call(
        body,
        out_shape=out,
        in_specs=ins,
        out_specs=to(),
        scratch_shapes=scratch,
        cost_estimate=pl.CostEstimate(flops=flops, transcendentals=0, bytes_accessed=0),
        compiler_params=pltpu.CompilerParams(vmem_limit_bytes=mib * 1024 * 1024),
    )


def dot_nn(a, b):
    return lax.dot_general(a, b, (((1,), (0,)), ((), ())), preferred_element_type=F32)


def dot_nt(a, b):
    return lax.dot_general(a, b, (((1,), (1,)), ((), ())), preferred_element_type=F32)


def pick_body(idx_ref, tok_ref, out_ref):
    caps, rows = idx_ref.shape[0], tok_ref.shape[0]
    hot = (lax.broadcasted_iota(jnp.int32, (caps, rows), 1) == idx_ref[...]).astype(BF)
    width = tok_ref.shape[1] // out_ref.shape[0]
    pad = jnp.zeros((caps, out_ref.shape[2] - width), BF)
    for m in range(out_ref.shape[0]):
        out_ref[m, :, :width] = dot_nn(hot, tok_ref[:, m * width : (m + 1) * width]).astype(BF)
        out_ref[m, :, width:] = pad


def mix(ord_ref, src, wrefs, spots):
    width, acc = 192, None
    for wref, places in zip(wrefs, spots):
        pieces = len(places) // 4
        for n, k in enumerate(places):
            lo = (n % pieces) * width
            part = dot_nn(src[ord_ref[k], :, :width], wref[n // pieces, lo : lo + width, :])
            acc = part if acc is None else acc + part
    return acc


def early_body(ord_ref, own_ref, mate_ref, ab_ref, out_ref):
    caps = own_ref.shape[1]
    spots = ([4 * q + n for q in range(4) for n in (0, 1)],)
    for n, src in enumerate((own_ref, mate_ref)):
        out_ref[n * caps : (n + 1) * caps, :] = mix(ord_ref, src, (ab_ref,), spots)


def hidden_body(ord_ref, own_ref, mate_ref, early_ref, c_ref, out_ref, res_ref, sems):
    caps = own_ref.shape[1]
    core = ord_ref[32]
    spots = ([4 * q + n for q in range(4) for n in (2, 3)],)
    for n, src in enumerate((own_ref, mate_ref)):
        acc = early_ref[n * caps : (n + 1) * caps, :] + mix(ord_ref, src, (c_ref,), spots)
        cols = []
        for s in range(2):
            gate = acc[:, 256 * s : 256 * s + 128]
            up = acc[:, 256 * s + 128 : 256 * s + 256]
            cols.append((gate / (1.0 + jnp.exp(-gate)) * up).astype(BF))
        at = pl.multiple_of((core if n == 0 else 1 - core) * caps, caps)
        res_ref[pl.ds(at, caps), :] = jnp.concatenate(cols, axis=1)
    copies = [pltpu.make_async_copy(res_ref, out_ref.at[g], sems.at[g]) for g in range(4)]
    for copy in copies:
        copy.start()
    for copy in copies:
        copy.wait()


def down_body(ord_ref, idx_ref, first_ref, second_ref, hid_ref, mate_ref, out_ref, scr, second_vmem, sem):
    caps = idx_ref.shape[1]
    rows, unit = 512, 24
    fetch = pltpu.make_async_copy(second_ref, second_vmem, sem)
    fetch.start()
    for n, w_ref in enumerate((first_ref, second_vmem)):
        if n == 1:
            fetch.wait()
        acc = None
        for core, h_ref in ((ord_ref[32], hid_ref), (1 - ord_ref[32], mate_ref)):
            for x in range(4):
                lo = pl.multiple_of(512 * x + 256 * core, 256)
                part = dot_nt(w_ref[:, pl.ds(lo, 256)], h_ref[x])
                acc = part if acc is None else acc + part
        for k in range(8):
            at = pl.multiple_of(ord_ref[16 + 8 * n + k] * unit, 8)
            scr[pl.ds(at, unit), :] = acc[k * unit : (k + 1) * unit, :]
    for b in range(2):
        hot = (lax.broadcasted_iota(jnp.int32, (rows, caps), 0) == idx_ref[b : b + 1, :]).astype(BF)
        dense = dot_nt(hot, scr[:, b * caps : (b + 1) * caps].astype(BF)).astype(BF)
        for n in range(16):
            out_ref[16 * b + n] = dense[32 * n : 32 * n + 32, :]


def spread_body(*refs):
    out_ref, sems = refs[-2], refs[-1]
    lo, copies = 0, []
    for n, r in enumerate(refs[:-2]):
        for q in range(out_ref.shape[0]):
            copies.append(pltpu.make_async_copy(r, out_ref.at[q, pl.ds(lo, r.shape[0])], sems.at[n, q]))
        lo += r.shape[0]
    for copy in copies:
        copy.start()
    for copy in copies:
        copy.wait()


def quarter_body(in_ref, out_ref):
    for x in range(4):
        out_ref[:, 512 * x : 512 * (x + 1)] = in_ref[24 * x : 24 * (x + 1), :]


def place_body(in_ref, scale_ref, out_ref, scr):
    unit = 24
    for g in range(8):
        core, x = g // 4, g % 4
        acc = in_ref[16 * core + x].astype(F32)
        for q in range(1, 4):
            acc = acc + in_ref[16 * core + 4 * q + x].astype(F32)
        turned = acc.T
        for m in range(16):
            lo = 192 * m + 96 * core + unit * x
            scr[lo : lo + unit, :] = turned[m * unit : (m + 1) * unit, :]
    for n in range(6):
        out_ref[:, n * 512 : (n + 1) * 512] = (scr[n * 512 : (n + 1) * 512, :].T * scale_ref[...]).astype(BF)


def pairs(step):
    flips = ((1, 3), (3, 1))
    return [(2 * i + c, 2 * (i ^ flips[c][step]) + c) for i in range(4) for c in range(2)]


def join_body(a_ref, b_ref, out_ref):
    rows = a_ref.shape[0]
    out_ref[:rows, :] = a_ref[...]
    out_ref[rows:, :] = b_ref[...]


def join(a, b):
    out = jax.ShapeDtypeStruct((a.shape[0] + b.shape[0], a.shape[1]), BF)
    return call(join_body, out, [vm(), vm()], mib=4)(a, b)


def meet(value, axis, step):
    return lax.ppermute(value, (axis, "c"), pairs(step))


def over_y(parts):
    rows, cols = sum(p.shape[0] for p in parts), parts[0].shape[1]
    wide = call(
        spread_body,
        pltpu.HBM((4, rows, cols), BF),
        [vm()] * len(parts),
        scratch=[pltpu.SemaphoreType.DMA((len(parts), 4))],
        mib=4,
        to=hb,
    )(*parts)
    return lax.all_to_all(wide, "y", 0, 0, tiled=True)


def shards(tokens, expert_ids, route_weight, index_list, gate_weight, up_weight, down_weight):
    zh, y, c, zl, x = (lax.axis_index(n) for n in ("zh", "y", "c", "zl", "x"))
    caps = index_list.shape[1]

    cut = lambda w, n: w[:, 128 * n : 128 * n + 128]
    mine = [
        jnp.concatenate([cut(w, 2 * h + s) for s in range(2) for w in (gate_weight, up_weight)], axis=1)
        for h in range(2)
    ]
    both_rows = lax.all_to_all(jnp.concatenate(mine, axis=0), "c", 0, 0, tiled=True)

    turned = down_weight.T
    quarter = lax.all_to_all(turned, "x", 0, 0, tiled=True)
    quarter = call(quarter_body, jax.ShapeDtypeStruct((24, 2048), BF), [vm()], mib=4)(quarter)

    flip = jnp.where(c == 0, jnp.array([0, 1, 3, 2]), jnp.array([0, 3, 1, 2])).astype(jnp.int32)
    order = ((zh ^ flip)[None, :] * 4 + jnp.arange(4, dtype=jnp.int32)[:, None]).reshape(16)
    order_down = ((zh ^ flip)[None, :] * 4 + (y ^ flip)[:, None]).reshape(16)
    order = jnp.concatenate([order, order_down, c.reshape(1)]).astype(jnp.int32)

    rows = call(
        pick_body, jax.ShapeDtypeStruct((16, caps, 256), BF), [vm(), vm()], flops=2 * 256 * 512 * 3072
    )(index_list.reshape(caps, 1), tokens)
    swap = [(0, 1), (1, 0)]
    rows_mate = lax.ppermute(rows, "c", swap)
    index_mate = lax.ppermute(index_list, "c", swap)
    index_both = jnp.where(
        c == 0,
        jnp.concatenate([index_list, index_mate], axis=0),
        jnp.concatenate([index_mate, index_list], axis=0),
    )

    near = meet(both_rows, "zh", 0)
    both = join(both_rows, near)
    far = meet(both, "zh", 1)
    yab = over_y((both,))
    yc = over_y((far,))

    near = meet(quarter, "zh", 0)
    two = join(quarter, near)
    far = meet(two, "zh", 1)
    four = join(two, far)
    near = meet(four, "y", 0)
    down_first = join(four, near)
    down_second = meet(down_first, "y", 1)

    early = call(
        early_body, jax.ShapeDtypeStruct((512, 512), F32), [sm()] + [vm()] * 3, flops=512 * 3072 * 512
    )(order, rows, rows_mate, yab)
    wide = call(
        hidden_body, pltpu.HBM((4, 512, 256), BF), [sm()] + [vm()] * 4, flops=512 * 3072 * 512,
        scratch=[pltpu.VMEM((512, 256), BF), pltpu.SemaphoreType.DMA((4,))], to=hb,
    )(order, rows, rows_mate, early, yc)
    hid = lax.all_to_all(wide, "x", 0, 0, tiled=True)
    hid_mate = lax.ppermute(hid, "c", swap)

    parts = call(
        down_body,
        jax.ShapeDtypeStruct((32, 32, 384), BF),
        [sm(), vm(), vm(), hb(), vm(), vm()],
        scratch=[pltpu.VMEM((384, 512), F32), pltpu.VMEM((192, 2048), BF), pltpu.SemaphoreType.DMA],
        flops=2 * 512 * 384 * 2048,
    )(order, index_both, down_first, down_second, hid, hid_mate)
    owned = lax.all_to_all(parts, ("c", "zl", "x"), 0, 0, tiled=True)

    start = (zl * 4 + x) * 32
    ids = lax.dynamic_slice_in_dim(expert_ids, start, 32, 0)
    weights = lax.dynamic_slice_in_dim(route_weight, start, 32, 0)
    scale = jnp.sum(jnp.where(ids == 0, weights, jnp.zeros_like(weights)), axis=1, keepdims=True)
    return call(
        place_body, jax.ShapeDtypeStruct((32, 3072), BF), [vm(), vm()], mib=8, scratch=[pltpu.VMEM((3072, 32), F32)]
    )(owned, scale)


def solution(mesh):
    fine = Mesh(mesh.devices.reshape(4, 4, 2, 4, 4), ("zh", "y", "c", "zl", "x"))
    edp, etp = ("zh", "y", "c"), ("zl", "x")
    in_specs = (P(edp, None), P(edp, None), P(edp, None), P(edp, None), P(edp, etp), P(edp, etp), P(etp, edp))

    return jax.shard_map(shards, mesh=fine, in_specs=in_specs, out_specs=P(edp + etp, None), check_vma=False)
```

```python
import jax
import jax.numpy as jnp
from jax import lax
from jax.experimental import pallas as pl
from jax.experimental.pallas import tpu as pltpu
from jax.sharding import Mesh, PartitionSpec as P


BF = jnp.bfloat16
F32 = jnp.float32


def vm():
    return pl.BlockSpec(memory_space=pltpu.VMEM)


def sm():
    return pl.BlockSpec(memory_space=pltpu.SMEM)


def hb():
    return pl.BlockSpec(memory_space=pltpu.HBM)


def call(body, out, ins, scratch=(), flops=0, mib=16, to=vm):
    return pl.pallas_call(
        body,
        out_shape=out,
        in_specs=ins,
        out_specs=[to(), to()] if isinstance(out, list) else to(),
        scratch_shapes=scratch,
        cost_estimate=pl.CostEstimate(flops=flops, transcendentals=0, bytes_accessed=0),
        compiler_params=pltpu.CompilerParams(vmem_limit_bytes=mib * 1024 * 1024),
    )


def dot_nn(a, b):
    return lax.dot_general(a, b, (((1,), (0,)), ((), ())), preferred_element_type=F32)


def dot_nt(a, b):
    return lax.dot_general(a, b, (((1,), (1,)), ((), ())), preferred_element_type=F32)


def pick_body(idx_ref, tok_ref, out_ref):
    caps, rows = idx_ref.shape[0], tok_ref.shape[0]
    hot = (lax.broadcasted_iota(jnp.int32, (caps, rows), 1) == idx_ref[...]).astype(BF)
    width = tok_ref.shape[1] // out_ref.shape[0]
    pad = jnp.zeros((caps, out_ref.shape[2] - width), BF)
    for m in range(out_ref.shape[0]):
        out_ref[m, :, :width] = dot_nn(hot, tok_ref[:, m * width : (m + 1) * width]).astype(BF)
        out_ref[m, :, width:] = pad


def lay(ord_ref, own_ref, mate_ref, out_ref, places):
    caps, width = own_ref.shape[1], 192
    for i, k in enumerate(places):
        out_ref[:caps, i * width : (i + 1) * width] = own_ref[ord_ref[k], :, :width]
        out_ref[caps:, i * width : (i + 1) * width] = mate_ref[ord_ref[k], :, :width]


def early_body(ord_ref, own_ref, mate_ref, a_ref, b_ref, out_ref, late_ref, now_ref, then_ref, sum_ref, sems):
    lay(ord_ref, own_ref, mate_ref, then_ref, [4 * q + n for q in range(4) for n in (2, 3)])
    copy = pltpu.make_async_copy(then_ref, late_ref, sems.at[0])
    copy.start()
    lay(ord_ref, own_ref, mate_ref, now_ref, [4 * q + n for n in (0, 1) for q in range(4)])
    half = a_ref.shape[0]
    sum_ref[...] = dot_nn(now_ref[:, :half], a_ref[...]) + dot_nn(now_ref[:, half:], b_ref[...])
    store = pltpu.make_async_copy(sum_ref, out_ref, sems.at[1])
    store.start()
    copy.wait()
    store.wait()


def hidden_body(ord_ref, rows_ref, early_ref, c_ref, out_ref, res_ref, rows_vmem, sum_ref, sems, out_sems):
    caps = rows_ref.shape[0] // 2
    half = rows_ref.shape[1] // 2
    core = ord_ref[32]
    copies = [
        pltpu.make_async_copy(rows_ref.at[:, pl.ds(n * half, half)], rows_vmem.at[:, pl.ds(n * half, half)], sems.at[n])
        for n in range(2)
    ] + [pltpu.make_async_copy(early_ref, sum_ref, sems.at[2])]
    for copy in copies:
        copy.start()
    acc = None
    for n in range(2):
        copies[n].wait()
        part = dot_nn(rows_vmem[:, n * half : (n + 1) * half], c_ref[n * half : (n + 1) * half, :])
        acc = part if acc is None else acc + part
    copies[2].wait()
    acc = acc + sum_ref[...]
    cols = []
    for s in range(2):
        gate = acc[:, 256 * s : 256 * s + 128]
        up = acc[:, 256 * s + 128 : 256 * s + 256]
        cols.append((gate / (1.0 + jnp.exp(-gate)) * up).astype(BF))
    res = jnp.concatenate(cols, axis=1)
    res_ref[pl.ds(pl.multiple_of(core * caps, caps), caps), :] = res[:caps]
    res_ref[pl.ds(pl.multiple_of((1 - core) * caps, caps), caps), :] = res[caps:]
    copies = [pltpu.make_async_copy(res_ref, out_ref.at[g], out_sems.at[g]) for g in range(4)]
    for copy in copies:
        copy.start()
    for copy in copies:
        copy.wait()


def down_body(ord_ref, idx_ref, first_ref, second_ref, hid_ref, mate_ref, out_ref, scr, w_ref, sems):
    caps = idx_ref.shape[1]
    rows, unit, acc = 512, 24, None
    copies = [
        pltpu.make_async_copy(r, w_ref.at[pl.ds(192 * n, 192)], sems.at[n]) for n, r in enumerate((first_ref, second_ref))
    ]
    for copy in copies:
        copy.start()
    for copy in copies:
        copy.wait()
    for core, h_ref in ((ord_ref[32], hid_ref), (1 - ord_ref[32], mate_ref)):
        for x in range(4):
            lo = pl.multiple_of(512 * x + 256 * core, 256)
            part = dot_nt(w_ref[:, pl.ds(lo, 256)], h_ref[x])
            acc = part if acc is None else acc + part
    for k in range(16):
        at = pl.multiple_of(ord_ref[16 + k] * unit, 8)
        scr[pl.ds(at, unit), :] = acc[k * unit : (k + 1) * unit, :]
    for b in range(2):
        hot = (lax.broadcasted_iota(jnp.int32, (rows, caps), 0) == idx_ref[b : b + 1, :]).astype(BF)
        dense = dot_nt(hot, scr[:, b * caps : (b + 1) * caps].astype(BF)).astype(BF)
        for n in range(16):
            out_ref[16 * b + n] = dense[32 * n : 32 * n + 32, :]


def spread_body(*refs):
    out_ref, sems = refs[-2], refs[-1]
    lo, copies = 0, []
    for n, r in enumerate(refs[:-2]):
        rows = min(r.shape[0], out_ref.shape[1] - lo)
        for q in range(out_ref.shape[0]):
            copies.append(
                pltpu.make_async_copy(r.at[pl.ds(0, rows)], out_ref.at[q, pl.ds(lo, rows)], sems.at[n, q])
            )
        lo += rows
    for copy in copies:
        copy.start()
    for copy in copies:
        copy.wait()


def quarter_body(own_ref, got_ref, out_ref):
    lo = got_ref.shape[0] - 96
    for x in range(4):
        out_ref[:24, 512 * x : 512 * (x + 1)] = own_ref[24 * x : 24 * (x + 1), :]
        out_ref[24:, 512 * x : 512 * (x + 1)] = got_ref[lo + 24 * x : lo + 24 * (x + 1), :]


def place_body(in_ref, scale_ref, out_ref, scr):
    unit = 24
    for g in range(8):
        core, x = g // 4, g % 4
        acc = in_ref[16 * core + x].astype(F32)
        for q in range(1, 4):
            acc = acc + in_ref[16 * core + 4 * q + x].astype(F32)
        turned = acc.T
        for m in range(16):
            lo = 192 * m + 96 * core + unit * x
            scr[lo : lo + unit, :] = turned[m * unit : (m + 1) * unit, :]
    for n in range(6):
        out_ref[:, n * 512 : (n + 1) * 512] = (scr[n * 512 : (n + 1) * 512, :].T * scale_ref[...]).astype(BF)


def pairs(step):
    flips = ((1, 3), (3, 1))
    return [(2 * i + c, 2 * (i ^ flips[c][step]) + c) for i in range(4) for c in range(2)]


def join_body(*refs):
    lo = 0
    for r in refs[:-1]:
        refs[-1][lo : lo + r.shape[0], :] = r[...]
        lo += r.shape[0]


def join(parts):
    out = jax.ShapeDtypeStruct((sum(p.shape[0] for p in parts), parts[0].shape[1]), BF)
    return call(join_body, out, [vm()] * len(parts), mib=4)(*parts)


def meet(value, axis, step):
    return lax.ppermute(value, (axis, "c"), pairs(step))


def over_y(parts, rows):
    cols = parts[0].shape[1]
    wide = call(
        spread_body,
        pltpu.HBM((4, rows, cols), BF),
        [vm()] * len(parts),
        scratch=[pltpu.SemaphoreType.DMA((len(parts), 4))],
        mib=4,
        to=hb,
    )(*parts)
    return lax.all_to_all(wide, "y", 0, 0, tiled=True)


def shards(tokens, expert_ids, route_weight, index_list, gate_weight, up_weight, down_weight):
    zh, y, c, zl, x = (lax.axis_index(n) for n in ("zh", "y", "c", "zl", "x"))
    caps = index_list.shape[1]

    cut = lambda w, n: w[:, 128 * n : 128 * n + 128]
    mine = [
        jnp.concatenate([cut(w, 2 * h + s) for s in range(2) for w in (gate_weight, up_weight)], axis=1)
        for h in range(2)
    ]
    both_rows = lax.all_to_all(jnp.concatenate(mine, axis=0), "c", 0, 0, tiled=True)

    turned = down_weight.T
    quarter = lax.all_to_all(turned, "x", 0, 0, tiled=True)
    flip = jnp.where(c == 0, jnp.array([0, 1, 3, 2]), jnp.array([0, 3, 1, 2])).astype(jnp.int32)
    order = ((zh ^ flip)[None, :] * 4 + jnp.arange(4, dtype=jnp.int32)[:, None]).reshape(16)
    turned_flip = jnp.where(c == 0, jnp.array([0, 3, 1, 2]), jnp.array([0, 1, 3, 2])).astype(jnp.int32)
    order_down = ((zh ^ turned_flip)[None, :] * 4 + (y ^ flip)[:, None]).reshape(16)
    order = jnp.concatenate([order, order_down, c.reshape(1)]).astype(jnp.int32)

    rows = call(
        pick_body, jax.ShapeDtypeStruct((16, caps, 256), BF), [vm(), vm()], flops=2 * 256 * 512 * 3072
    )(index_list.reshape(caps, 1), tokens)
    swap = [(0, 1), (1, 0)]
    rows_mate = lax.ppermute(rows, "c", swap)
    index_mate = lax.ppermute(index_list, "c", swap)
    index_both = jnp.where(
        c == 0,
        jnp.concatenate([index_list, index_mate], axis=0),
        jnp.concatenate([index_mate, index_list], axis=0),
    )

    near = meet(both_rows, "zh", 0)
    ya = over_y((both_rows,), 192)
    yb = over_y((near,), 192)
    far = meet(join((both_rows, near, quarter)), "zh", 1)
    yc = over_y((far,), 384)
    ya, yb, yc = ya.reshape(768, 512), yb.reshape(768, 512), yc.reshape(1536, 512)

    two = call(quarter_body, jax.ShapeDtypeStruct((48, 2048), BF), [vm()] * 2, mib=4)(quarter, far)
    far = pltpu.with_memory_space_constraint(meet(two, "zh", 0), pltpu.HBM)
    four = join((two, far))
    near = pltpu.with_memory_space_constraint(meet(four, "y", 0), pltpu.HBM)
    down_first = join((four, near))
    down_second = meet(down_first, "y", 1)

    early, rows_late = call(
        early_body,
        [pltpu.HBM((512, 512), F32), pltpu.HBM((512, 1536), BF)],
        [sm()] + [vm()] * 4,
        scratch=[pltpu.VMEM((512, 1536), BF)] * 2 + [pltpu.VMEM((512, 512), F32), pltpu.SemaphoreType.DMA((2,))],
        flops=512 * 3072 * 512,
        to=hb,
    )(order, rows, rows_mate, ya, yb)
    early, rows_late = (pltpu.with_memory_space_constraint(v, pltpu.HBM) for v in (early, rows_late))
    wide = call(
        hidden_body,
        pltpu.HBM((4, 512, 256), BF),
        [sm(), hb(), hb(), vm()],
        scratch=[
            pltpu.VMEM((512, 256), BF),
            pltpu.VMEM((512, 1536), BF),
            pltpu.VMEM((512, 512), F32),
            pltpu.SemaphoreType.DMA((3,)),
            pltpu.SemaphoreType.DMA((4,)),
        ],
        flops=512 * 3072 * 512,
        to=hb,
    )(order, rows_late, early, yc)
    hid = lax.all_to_all(wide, "x", 0, 0, tiled=True)
    hid_mate = lax.ppermute(hid, "c", swap)

    parts = call(
        down_body,
        jax.ShapeDtypeStruct((32, 32, 384), BF),
        [sm(), vm(), hb(), hb(), vm(), vm()],
        scratch=[pltpu.VMEM((384, 512), F32), pltpu.VMEM((384, 2048), BF), pltpu.SemaphoreType.DMA((2,))],
        flops=2 * 512 * 384 * 2048,
    )(order, index_both, down_first, down_second, hid, hid_mate)
    owned = lax.all_to_all(parts, ("c", "zl", "x"), 0, 0, tiled=True)

    start = (zl * 4 + x) * 32
    ids = lax.dynamic_slice_in_dim(expert_ids, start, 32, 0)
    weights = lax.dynamic_slice_in_dim(route_weight, start, 32, 0)
    scale = jnp.sum(jnp.where(ids == 0, weights, jnp.zeros_like(weights)), axis=1, keepdims=True)
    return call(
        place_body, jax.ShapeDtypeStruct((32, 3072), BF), [vm(), vm()], mib=8, scratch=[pltpu.VMEM((3072, 32), F32)]
    )(owned, scale)


def solution(mesh):
    fine = Mesh(mesh.devices.reshape(4, 4, 2, 4, 4), ("zh", "y", "c", "zl", "x"))
    edp, etp = ("zh", "y", "c"), ("zl", "x")
    in_specs = (P(edp, None), P(edp, None), P(edp, None), P(edp, None), P(edp, etp), P(edp, etp), P(etp, edp))

    return jax.shard_map(shards, mesh=fine, in_specs=in_specs, out_specs=P(edp + etp, None), check_vma=False)
```

```python
import jax
import jax.numpy as jnp
from jax import lax
from jax.experimental import pallas as pl
from jax.experimental.pallas import tpu as pltpu
from jax.sharding import Mesh, PartitionSpec as P


BF = jnp.bfloat16
F32 = jnp.float32


def vm():
    return pl.BlockSpec(memory_space=pltpu.VMEM)


def sm():
    return pl.BlockSpec(memory_space=pltpu.SMEM)


def hb():
    return pl.BlockSpec(memory_space=pltpu.HBM)


def call(body, out, ins, scratch=(), flops=0, mib=16, to=vm):
    return pl.pallas_call(
        body,
        out_shape=out,
        in_specs=ins,
        out_specs=[to(), to()] if isinstance(out, list) else to(),
        scratch_shapes=scratch,
        cost_estimate=pl.CostEstimate(flops=flops, transcendentals=0, bytes_accessed=0),
        compiler_params=pltpu.CompilerParams(vmem_limit_bytes=mib * 1024 * 1024),
    )


def dot_nn(a, b):
    return lax.dot_general(a, b, (((1,), (0,)), ((), ())), preferred_element_type=F32)


def dot_nt(a, b):
    return lax.dot_general(a, b, (((1,), (1,)), ((), ())), preferred_element_type=F32)


def pick_body(idx_ref, tok_ref, out_ref):
    caps, rows = idx_ref.shape[0], tok_ref.shape[0]
    hot = (lax.broadcasted_iota(jnp.int32, (caps, rows), 1) == idx_ref[...]).astype(BF)
    width = tok_ref.shape[1] // out_ref.shape[0]
    pad = jnp.zeros((caps, out_ref.shape[2] - width), BF)
    for m in range(out_ref.shape[0]):
        out_ref[m, :, :width] = dot_nn(hot, tok_ref[:, m * width : (m + 1) * width]).astype(BF)
        out_ref[m, :, width:] = pad


def lay(ord_ref, own_ref, mate_ref, out_ref, places):
    caps, width = own_ref.shape[1], 192
    for i, k in enumerate(places):
        out_ref[:caps, i * width : (i + 1) * width] = own_ref[ord_ref[k], :, :width]
        out_ref[caps:, i * width : (i + 1) * width] = mate_ref[ord_ref[k], :, :width]


def early_body(ord_ref, own_ref, mate_ref, *rest):
    piece_refs, (out_ref, late_ref, now_ref, then_ref, sum_ref, sems) = rest[:4], rest[4:]
    lay(ord_ref, own_ref, mate_ref, then_ref, [4 * q + n for q in range(4) for n in (2, 3)])
    copy = pltpu.make_async_copy(then_ref, late_ref, sems.at[0])
    copy.start()
    lay(ord_ref, own_ref, mate_ref, now_ref, [4 * q + n for q in range(4) for n in (0, 1)])
    acc = None
    for q, piece in enumerate(piece_refs):
        part = dot_nn(now_ref[:, 384 * q : 384 * (q + 1)], piece[...])
        acc = part if acc is None else acc + part
    sum_ref[...] = acc
    store = pltpu.make_async_copy(sum_ref, out_ref, sems.at[1])
    store.start()
    copy.wait()
    store.wait()


def hidden_body(ord_ref, rows_ref, early_ref, *rest):
    piece_refs, (out_ref, res_ref, rows_vmem, sum_ref, sems, out_sems) = rest[:4], rest[4:]
    caps = rows_ref.shape[0] // 2
    half = rows_ref.shape[1] // 2
    core = ord_ref[16]
    copies = [
        pltpu.make_async_copy(rows_ref.at[:, pl.ds(n * half, half)], rows_vmem.at[:, pl.ds(n * half, half)], sems.at[n])
        for n in range(2)
    ] + [pltpu.make_async_copy(early_ref, sum_ref, sems.at[2])]
    for copy in copies:
        copy.start()
    acc = None
    for n in range(2):
        copies[n].wait()
        for q in (2 * n, 2 * n + 1):
            part = dot_nn(rows_vmem[:, 384 * q : 384 * (q + 1)], piece_refs[q][...])
            acc = part if acc is None else acc + part
    copies[2].wait()
    acc = acc + sum_ref[...]
    cols = []
    for s in range(2):
        gate = acc[:, 256 * s : 256 * s + 128]
        up = acc[:, 256 * s + 128 : 256 * s + 256]
        cols.append((gate / (1.0 + jnp.exp(-gate)) * up).astype(BF))
    res = jnp.concatenate(cols, axis=1)
    res_ref[pl.ds(pl.multiple_of(core * caps, caps), caps), :] = res[:caps]
    res_ref[pl.ds(pl.multiple_of((1 - core) * caps, caps), caps), :] = res[caps:]
    copies = [pltpu.make_async_copy(res_ref, out_ref.at[g], out_sems.at[g]) for g in range(4)]
    for copy in copies:
        copy.start()
    for copy in copies:
        copy.wait()


def down_body(ord_ref, idx_ref, *rest):
    piece_refs, (hid_ref, mate_ref, out_ref, scr, w_ref, sems) = rest[:4], rest[4:]
    caps = idx_ref.shape[1]
    rows, unit, acc = 512, 24, None
    copies = [
        pltpu.make_async_copy(r, w_ref.at[pl.ds(96 * n, 96)], sems.at[n]) for n, r in enumerate(piece_refs)
    ]
    for copy in copies:
        copy.start()
    for copy in copies:
        copy.wait()
    for core, h_ref in ((ord_ref[16], hid_ref), (1 - ord_ref[16], mate_ref)):
        for x in range(4):
            lo = pl.multiple_of(512 * x + 256 * core, 256)
            part = dot_nt(w_ref[:, pl.ds(lo, 256)], h_ref[x])
            acc = part if acc is None else acc + part
    for k in range(16):
        at = pl.multiple_of(ord_ref[k] * unit, 8)
        scr[pl.ds(at, unit), :] = acc[k * unit : (k + 1) * unit, :]
    for b in range(2):
        hot = (lax.broadcasted_iota(jnp.int32, (rows, caps), 0) == idx_ref[b : b + 1, :]).astype(BF)
        dense = dot_nt(hot, scr[:, b * caps : (b + 1) * caps].astype(BF)).astype(BF)
        for n in range(16):
            out_ref[16 * b + n] = dense[32 * n : 32 * n + 32, :]


def quarter_body(in_ref, out_ref):
    for x in range(4):
        out_ref[:, 512 * x : 512 * (x + 1)] = in_ref[24 * x : 24 * (x + 1), :]


def place_body(in_ref, scale_ref, out_ref, scr):
    unit = 24
    for g in range(8):
        core, x = g // 4, g % 4
        acc = in_ref[16 * core + x].astype(F32)
        for q in range(1, 4):
            acc = acc + in_ref[16 * core + 4 * q + x].astype(F32)
        turned = acc.T
        for m in range(16):
            lo = 192 * m + 96 * core + unit * x
            scr[lo : lo + unit, :] = turned[m * unit : (m + 1) * unit, :]
    for n in range(6):
        out_ref[:, n * 512 : (n + 1) * 512] = (scr[n * 512 : (n + 1) * 512, :].T * scale_ref[...]).astype(BF)


def pairs(step):
    flips = ((1, 3), (3, 1))
    return [(2 * i + c, 2 * (i ^ flips[c][step]) + c) for i in range(4) for c in range(2)]


def join_body(*refs):
    lo = 0
    for r in refs[:-1]:
        refs[-1][lo : lo + r.shape[0], :] = r[...]
        lo += r.shape[0]


def join(parts):
    out = jax.ShapeDtypeStruct((sum(p.shape[0] for p in parts), parts[0].shape[1]), BF)
    return call(join_body, out, [vm()] * len(parts), mib=4)(*parts)


def meet(value, axis, step):
    return lax.ppermute(value, (axis, "c"), pairs(step))


def over_y(value):
    near = meet(value, "y", 0)
    other = meet(value, "y", 1)
    return value, near, other, meet(near, "y", 1)


def shards(tokens, expert_ids, route_weight, index_list, gate_weight, up_weight, down_weight):
    zh, y, c, zl, x = (lax.axis_index(n) for n in ("zh", "y", "c", "zl", "x"))
    caps = index_list.shape[1]

    cut = lambda w, n: w[:, 128 * n : 128 * n + 128]
    mine = [
        jnp.concatenate([cut(w, 2 * h + s) for s in range(2) for w in (gate_weight, up_weight)], axis=1)
        for h in range(2)
    ]
    both_rows = lax.all_to_all(jnp.concatenate(mine, axis=0), "c", 0, 0, tiled=True)

    turned = down_weight.T
    quarter = lax.all_to_all(turned, "x", 0, 0, tiled=True)
    quarter = call(quarter_body, jax.ShapeDtypeStruct((24, 2048), BF), [vm()], mib=4)(quarter)

    flip = jnp.where(c == 0, jnp.array([0, 1, 3, 2]), jnp.array([0, 3, 1, 2])).astype(jnp.int32)
    order = ((zh ^ flip)[None, :] * 4 + (y ^ flip)[:, None]).reshape(16)
    order = jnp.concatenate([order, c.reshape(1)]).astype(jnp.int32)

    rows = call(
        pick_body, jax.ShapeDtypeStruct((16, caps, 256), BF), [vm(), vm()], flops=2 * 256 * 512 * 3072
    )(index_list.reshape(caps, 1), tokens)
    swap = [(0, 1), (1, 0)]
    rows_mate = lax.ppermute(rows, "c", swap)
    index_mate = lax.ppermute(index_list, "c", swap)
    index_both = jnp.where(
        c == 0,
        jnp.concatenate([index_list, index_mate], axis=0),
        jnp.concatenate([index_mate, index_list], axis=0),
    )

    near = meet(both_rows, "zh", 0)
    both = join((both_rows, near))
    far = meet(both, "zh", 1)
    soon = over_y(both)
    later = over_y(far)

    near = pltpu.with_memory_space_constraint(meet(quarter, "zh", 0), pltpu.HBM)
    two = join((quarter, near))
    far = pltpu.with_memory_space_constraint(meet(two, "zh", 1), pltpu.HBM)
    downs = over_y(join((two, far)))

    early, rows_late = call(
        early_body,
        [pltpu.HBM((512, 512), F32), pltpu.HBM((512, 1536), BF)],
        [sm()] + [vm()] * 6,
        scratch=[pltpu.VMEM((512, 1536), BF)] * 2 + [pltpu.VMEM((512, 512), F32), pltpu.SemaphoreType.DMA((2,))],
        flops=512 * 3072 * 512,
        to=hb,
    )(order, rows, rows_mate, *soon)
    early, rows_late = (pltpu.with_memory_space_constraint(v, pltpu.HBM) for v in (early, rows_late))
    wide = call(
        hidden_body,
        pltpu.HBM((4, 512, 256), BF),
        [sm(), hb(), hb()] + [vm()] * 4,
        scratch=[
            pltpu.VMEM((512, 256), BF),
            pltpu.VMEM((512, 1536), BF),
            pltpu.VMEM((512, 512), F32),
            pltpu.SemaphoreType.DMA((3,)),
            pltpu.SemaphoreType.DMA((4,)),
        ],
        flops=512 * 3072 * 512,
        to=hb,
    )(order, rows_late, early, *later)
    hid = lax.all_to_all(wide, "x", 0, 0, tiled=True)
    hid_mate = lax.ppermute(hid, "c", swap)

    parts = call(
        down_body,
        jax.ShapeDtypeStruct((32, 32, 384), BF),
        [sm(), vm()] + [hb()] * 4 + [vm()] * 2,
        scratch=[pltpu.VMEM((384, 512), F32), pltpu.VMEM((384, 2048), BF), pltpu.SemaphoreType.DMA((4,))],
        flops=2 * 512 * 384 * 2048,
    )(order, index_both, *downs, hid, hid_mate)
    owned = lax.all_to_all(parts, ("c", "zl", "x"), 0, 0, tiled=True)

    start = (zl * 4 + x) * 32
    ids = lax.dynamic_slice_in_dim(expert_ids, start, 32, 0)
    weights = lax.dynamic_slice_in_dim(route_weight, start, 32, 0)
    scale = jnp.sum(jnp.where(ids == 0, weights, jnp.zeros_like(weights)), axis=1, keepdims=True)
    return call(
        place_body, jax.ShapeDtypeStruct((32, 3072), BF), [vm(), vm()], mib=8, scratch=[pltpu.VMEM((3072, 32), F32)]
    )(owned, scale)


def solution(mesh):
    fine = Mesh(mesh.devices.reshape(4, 4, 2, 4, 4), ("zh", "y", "c", "zl", "x"))
    edp, etp = ("zh", "y", "c"), ("zl", "x")
    in_specs = (P(edp, None), P(edp, None), P(edp, None), P(edp, None), P(edp, etp), P(edp, etp), P(etp, edp))

    return jax.shard_map(shards, mesh=fine, in_specs=in_specs, out_specs=P(edp + etp, None), check_vma=False)
```

```python
import jax
import jax.numpy as jnp
from jax import lax
from jax.experimental import pallas as pl
from jax.experimental.pallas import tpu as pltpu
from jax.sharding import Mesh, PartitionSpec as P


BF = jnp.bfloat16
F32 = jnp.float32


def vm():
    return pl.BlockSpec(memory_space=pltpu.VMEM)


def sm():
    return pl.BlockSpec(memory_space=pltpu.SMEM)


def hb():
    return pl.BlockSpec(memory_space=pltpu.HBM)


def call(body, out, ins, scratch=(), flops=0, mib=16, to=vm):
    return pl.pallas_call(
        body,
        out_shape=out,
        in_specs=ins,
        out_specs=[to(), to()] if isinstance(out, list) else to(),
        scratch_shapes=scratch,
        cost_estimate=pl.CostEstimate(flops=flops, transcendentals=0, bytes_accessed=0),
        compiler_params=pltpu.CompilerParams(vmem_limit_bytes=mib * 1024 * 1024),
    )


def dot_nn(a, b):
    return lax.dot_general(a, b, (((1,), (0,)), ((), ())), preferred_element_type=F32)


def dot_nt(a, b):
    return lax.dot_general(a, b, (((1,), (1,)), ((), ())), preferred_element_type=F32)


def pick_body(idx_ref, tok_ref, out_ref):
    caps, rows = idx_ref.shape[0], tok_ref.shape[0]
    hot = (lax.broadcasted_iota(jnp.int32, (caps, rows), 1) == idx_ref[...]).astype(BF)
    width = tok_ref.shape[1] // out_ref.shape[0]
    pad = jnp.zeros((caps, out_ref.shape[2] - width), BF)
    for m in range(out_ref.shape[0]):
        out_ref[m, :, :width] = dot_nn(hot, tok_ref[:, m * width : (m + 1) * width]).astype(BF)
        out_ref[m, :, width:] = pad


def lay(ord_ref, own_ref, mate_ref, out_ref, first):
    caps, width = own_ref.shape[1], 192
    places = [4 * q + n for q in range(4) for n in (first, first + 1)]
    for i, k in enumerate(places):
        out_ref[:caps, i * width : (i + 1) * width] = own_ref[ord_ref[k], :, :width]
        out_ref[caps:, i * width : (i + 1) * width] = mate_ref[ord_ref[k], :, :width]


def early_body(ord_ref, own_ref, mate_ref, ab_ref, out_ref, late_ref, now_ref, then_ref, sum_ref, sems):
    lay(ord_ref, own_ref, mate_ref, then_ref, 2)
    copy = pltpu.make_async_copy(then_ref, late_ref, sems.at[0])
    copy.start()
    lay(ord_ref, own_ref, mate_ref, now_ref, 0)
    sum_ref[...] = dot_nn(now_ref[...], ab_ref[...])
    store = pltpu.make_async_copy(sum_ref, out_ref, sems.at[1])
    store.start()
    copy.wait()
    store.wait()


def hidden_body(ord_ref, rows_ref, early_ref, c_ref, out_ref, res_ref, rows_vmem, sum_ref, sems, out_sems):
    caps = rows_ref.shape[0] // 2
    half = rows_ref.shape[1] // 2
    core = ord_ref[32]
    copies = [
        pltpu.make_async_copy(rows_ref.at[:, pl.ds(n * half, half)], rows_vmem.at[:, pl.ds(n * half, half)], sems.at[n])
        for n in range(2)
    ] + [pltpu.make_async_copy(early_ref, sum_ref, sems.at[2])]
    for copy in copies:
        copy.start()
    acc = None
    for n in range(2):
        copies[n].wait()
        part = dot_nn(rows_vmem[:, n * half : (n + 1) * half], c_ref[n * half : (n + 1) * half, :])
        acc = part if acc is None else acc + part
    copies[2].wait()
    acc = acc + sum_ref[...]
    cols = []
    for s in range(2):
        gate = acc[:, 256 * s : 256 * s + 128]
        up = acc[:, 256 * s + 128 : 256 * s + 256]
        cols.append((gate / (1.0 + jnp.exp(-gate)) * up).astype(BF))
    res = jnp.concatenate(cols, axis=1)
    res_ref[pl.ds(pl.multiple_of(core * caps, caps), caps), :] = res[:caps]
    res_ref[pl.ds(pl.multiple_of((1 - core) * caps, caps), caps), :] = res[caps:]
    copies = [pltpu.make_async_copy(res_ref, out_ref.at[g], out_sems.at[g]) for g in range(4)]
    for copy in copies:
        copy.start()
    for copy in copies:
        copy.wait()


def down_body(ord_ref, idx_ref, first_ref, second_ref, hid_ref, mate_ref, out_ref, scr, w_ref, sems):
    caps = idx_ref.shape[1]
    rows, unit, acc = 512, 24, None
    copies = [
        pltpu.make_async_copy(r, w_ref.at[pl.ds(192 * n, 192)], sems.at[n]) for n, r in enumerate((first_ref, second_ref))
    ]
    for copy in copies:
        copy.start()
    for copy in copies:
        copy.wait()
    for core, h_ref in ((ord_ref[32], hid_ref), (1 - ord_ref[32], mate_ref)):
        for x in range(4):
            lo = pl.multiple_of(512 * x + 256 * core, 256)
            part = dot_nt(w_ref[:, pl.ds(lo, 256)], h_ref[x])
            acc = part if acc is None else acc + part
    for k in range(16):
        at = pl.multiple_of(ord_ref[16 + k] * unit, 8)
        scr[pl.ds(at, unit), :] = acc[k * unit : (k + 1) * unit, :]
    for b in range(2):
        hot = (lax.broadcasted_iota(jnp.int32, (rows, caps), 0) == idx_ref[b : b + 1, :]).astype(BF)
        dense = dot_nt(hot, scr[:, b * caps : (b + 1) * caps].astype(BF)).astype(BF)
        for n in range(16):
            out_ref[16 * b + n] = dense[32 * n : 32 * n + 32, :]


def spread_body(*refs):
    out_ref, sems = refs[-2], refs[-1]
    lo, copies = 0, []
    for n, r in enumerate(refs[:-2]):
        for q in range(out_ref.shape[0]):
            copies.append(pltpu.make_async_copy(r, out_ref.at[q, pl.ds(lo, r.shape[0])], sems.at[n, q]))
        lo += r.shape[0]
    for copy in copies:
        copy.start()
    for copy in copies:
        copy.wait()


def quarter_body(in_ref, out_ref):
    for x in range(4):
        out_ref[:, 512 * x : 512 * (x + 1)] = in_ref[24 * x : 24 * (x + 1), :]


def place_body(in_ref, scale_ref, out_ref, scr):
    unit = 24
    for g in range(8):
        core, x = g // 4, g % 4
        acc = in_ref[16 * core + x].astype(F32)
        for q in range(1, 4):
            acc = acc + in_ref[16 * core + 4 * q + x].astype(F32)
        turned = acc.T
        for m in range(16):
            lo = 192 * m + 96 * core + unit * x
            scr[lo : lo + unit, :] = turned[m * unit : (m + 1) * unit, :]
    for n in range(6):
        out_ref[:, n * 512 : (n + 1) * 512] = (scr[n * 512 : (n + 1) * 512, :].T * scale_ref[...]).astype(BF)


def pairs(step):
    flips = ((1, 3), (3, 1))
    return [(2 * i + c, 2 * (i ^ flips[c][step]) + c) for i in range(4) for c in range(2)]


def join_body(a_ref, b_ref, out_ref):
    rows = a_ref.shape[0]
    out_ref[:rows, :] = a_ref[...]
    out_ref[rows:, :] = b_ref[...]


def join(a, b):
    out = jax.ShapeDtypeStruct((a.shape[0] + b.shape[0], a.shape[1]), BF)
    return call(join_body, out, [vm(), vm()], mib=4)(a, b)


def meet(value, axis, step):
    return lax.ppermute(value, (axis, "c"), pairs(step))


def over_y(parts):
    rows, cols = sum(p.shape[0] for p in parts), parts[0].shape[1]
    wide = call(
        spread_body,
        pltpu.HBM((4, rows, cols), BF),
        [vm()] * len(parts),
        scratch=[pltpu.SemaphoreType.DMA((len(parts), 4))],
        mib=4,
        to=hb,
    )(*parts)
    return lax.all_to_all(wide, "y", 0, 0, tiled=True)


def shards(tokens, expert_ids, route_weight, index_list, gate_weight, up_weight, down_weight):
    zh, y, c, zl, x = (lax.axis_index(n) for n in ("zh", "y", "c", "zl", "x"))
    caps = index_list.shape[1]

    cut = lambda w, n: w[:, 128 * n : 128 * n + 128]
    mine = [
        jnp.concatenate([cut(w, 2 * h + s) for s in range(2) for w in (gate_weight, up_weight)], axis=1)
        for h in range(2)
    ]
    both_rows = lax.all_to_all(jnp.concatenate(mine, axis=0), "c", 0, 0, tiled=True)

    turned = down_weight.T
    quarter = lax.all_to_all(turned, "x", 0, 0, tiled=True)
    quarter = call(quarter_body, jax.ShapeDtypeStruct((24, 2048), BF), [vm()], mib=4)(quarter)

    flip = jnp.where(c == 0, jnp.array([0, 1, 3, 2]), jnp.array([0, 3, 1, 2])).astype(jnp.int32)
    order = ((zh ^ flip)[None, :] * 4 + jnp.arange(4, dtype=jnp.int32)[:, None]).reshape(16)
    order_down = ((zh ^ flip)[None, :] * 4 + (y ^ flip)[:, None]).reshape(16)
    order = jnp.concatenate([order, order_down, c.reshape(1)]).astype(jnp.int32)

    rows = call(
        pick_body, jax.ShapeDtypeStruct((16, caps, 256), BF), [vm(), vm()], flops=2 * 256 * 512 * 3072
    )(index_list.reshape(caps, 1), tokens)
    swap = [(0, 1), (1, 0)]
    rows_mate = lax.ppermute(rows, "c", swap)
    index_mate = lax.ppermute(index_list, "c", swap)
    index_both = jnp.where(
        c == 0,
        jnp.concatenate([index_list, index_mate], axis=0),
        jnp.concatenate([index_mate, index_list], axis=0),
    )

    near = meet(both_rows, "zh", 0)
    both = join(both_rows, near)
    far = meet(both, "zh", 1)
    yab = over_y((both,))
    yc = over_y((far,))

    near = meet(quarter, "zh", 0)
    two = join(quarter, near)
    far = pltpu.with_memory_space_constraint(meet(two, "zh", 1), pltpu.HBM)
    four = join(two, far)
    near = pltpu.with_memory_space_constraint(meet(four, "y", 0), pltpu.HBM)
    down_first = join(four, near)
    down_second = meet(down_first, "y", 1)

    yab, yc = yab.reshape(1536, 512), yc.reshape(1536, 512)
    early, rows_late = call(
        early_body,
        [pltpu.HBM((512, 512), F32), pltpu.HBM((512, 1536), BF)],
        [sm()] + [vm()] * 3,
        scratch=[pltpu.VMEM((512, 1536), BF)] * 2 + [pltpu.VMEM((512, 512), F32), pltpu.SemaphoreType.DMA((2,))],
        flops=512 * 3072 * 512,
        to=hb,
    )(order, rows, rows_mate, yab)
    early, rows_late = (pltpu.with_memory_space_constraint(v, pltpu.HBM) for v in (early, rows_late))
    wide = call(
        hidden_body,
        pltpu.HBM((4, 512, 256), BF),
        [sm(), hb(), hb(), vm()],
        scratch=[
            pltpu.VMEM((512, 256), BF),
            pltpu.VMEM((512, 1536), BF),
            pltpu.VMEM((512, 512), F32),
            pltpu.SemaphoreType.DMA((3,)),
            pltpu.SemaphoreType.DMA((4,)),
        ],
        flops=512 * 3072 * 512,
        to=hb,
    )(order, rows_late, early, yc)
    hid = lax.all_to_all(wide, "x", 0, 0, tiled=True)
    hid_mate = lax.ppermute(hid, "c", swap)

    parts = call(
        down_body,
        jax.ShapeDtypeStruct((32, 32, 384), BF),
        [sm(), vm(), hb(), hb(), vm(), vm()],
        scratch=[pltpu.VMEM((384, 512), F32), pltpu.VMEM((384, 2048), BF), pltpu.SemaphoreType.DMA((2,))],
        flops=2 * 512 * 384 * 2048,
    )(order, index_both, down_first, down_second, hid, hid_mate)
    owned = lax.all_to_all(parts, ("c", "zl", "x"), 0, 0, tiled=True)

    start = (zl * 4 + x) * 32
    ids = lax.dynamic_slice_in_dim(expert_ids, start, 32, 0)
    weights = lax.dynamic_slice_in_dim(route_weight, start, 32, 0)
    scale = jnp.sum(jnp.where(ids == 0, weights, jnp.zeros_like(weights)), axis=1, keepdims=True)
    return call(
        place_body, jax.ShapeDtypeStruct((32, 3072), BF), [vm(), vm()], mib=8, scratch=[pltpu.VMEM((3072, 32), F32)]
    )(owned, scale)


def solution(mesh):
    fine = Mesh(mesh.devices.reshape(4, 4, 2, 4, 4), ("zh", "y", "c", "zl", "x"))
    edp, etp = ("zh", "y", "c"), ("zl", "x")
    in_specs = (P(edp, None), P(edp, None), P(edp, None), P(edp, None), P(edp, etp), P(edp, etp), P(etp, edp))

    return jax.shard_map(shards, mesh=fine, in_specs=in_specs, out_specs=P(edp + etp, None), check_vma=False)
```

```python
import jax
import jax.numpy as jnp
from jax import lax
from jax.experimental import pallas as pl
from jax.experimental.pallas import tpu as pltpu
from jax.sharding import Mesh, PartitionSpec as P


BF = jnp.bfloat16
F32 = jnp.float32


def vm():
    return pl.BlockSpec(memory_space=pltpu.VMEM)


def sm():
    return pl.BlockSpec(memory_space=pltpu.SMEM)


def hb():
    return pl.BlockSpec(memory_space=pltpu.HBM)


def call(body, out, ins, scratch=(), flops=0, mib=16, to=vm):
    return pl.pallas_call(
        body,
        out_shape=out,
        in_specs=ins,
        out_specs=[to(), to()] if isinstance(out, list) else to(),
        scratch_shapes=scratch,
        cost_estimate=pl.CostEstimate(flops=flops, transcendentals=0, bytes_accessed=0),
        compiler_params=pltpu.CompilerParams(vmem_limit_bytes=mib * 1024 * 1024),
    )


def dot_nn(a, b):
    return lax.dot_general(a, b, (((1,), (0,)), ((), ())), preferred_element_type=F32)


def dot_nt(a, b):
    return lax.dot_general(a, b, (((1,), (1,)), ((), ())), preferred_element_type=F32)


def pick_body(idx_ref, tok_ref, out_ref):
    caps, rows = idx_ref.shape[0], tok_ref.shape[0]
    hot = (lax.broadcasted_iota(jnp.int32, (caps, rows), 1) == idx_ref[...]).astype(BF)
    width = tok_ref.shape[1] // out_ref.shape[0]
    pad = jnp.zeros((caps, out_ref.shape[2] - width), BF)
    for m in range(out_ref.shape[0]):
        out_ref[m, :, :width] = dot_nn(hot, tok_ref[:, m * width : (m + 1) * width]).astype(BF)
        out_ref[m, :, width:] = pad


def lay(ord_ref, own_ref, mate_ref, out_ref, places):
    caps, width = own_ref.shape[1], 192
    for i, k in enumerate(places):
        out_ref[:caps, i * width : (i + 1) * width] = own_ref[ord_ref[k], :, :width]
        out_ref[caps:, i * width : (i + 1) * width] = mate_ref[ord_ref[k], :, :width]


def early_body(ord_ref, own_ref, mate_ref, *rest):
    piece_refs, (out_ref, late_ref, now_ref, then_ref, sum_ref, sems) = rest[:4], rest[4:]
    lay(ord_ref, own_ref, mate_ref, then_ref, [4 * q + n for q in range(4) for n in (2, 3)])
    copy = pltpu.make_async_copy(then_ref, late_ref, sems.at[0])
    copy.start()
    lay(ord_ref, own_ref, mate_ref, now_ref, [16 + 4 * q + n for q in range(4) for n in (0, 1)])
    acc = None
    for q, piece in enumerate(piece_refs):
        part = dot_nn(now_ref[:, 384 * q : 384 * (q + 1)], piece[...])
        acc = part if acc is None else acc + part
    sum_ref[...] = acc
    store = pltpu.make_async_copy(sum_ref, out_ref, sems.at[1])
    store.start()
    copy.wait()
    store.wait()


def hidden_body(ord_ref, rows_ref, early_ref, c_ref, out_ref, res_ref, rows_vmem, c_vmem, sum_ref, sems, out_sems):
    caps = rows_ref.shape[0] // 2
    half = rows_ref.shape[1] // 2
    core = ord_ref[32]
    copies = []
    for n in range(2):
        cut = pl.ds(n * half, half)
        copies.append(pltpu.make_async_copy(rows_ref.at[:, cut], rows_vmem.at[:, cut], sems.at[2 * n]))
        copies.append(pltpu.make_async_copy(c_ref.at[cut], c_vmem.at[cut], sems.at[2 * n + 1]))
    copies.append(pltpu.make_async_copy(early_ref, sum_ref, sems.at[4]))
    for copy in copies:
        copy.start()
    acc = None
    for n in range(2):
        copies[2 * n].wait()
        copies[2 * n + 1].wait()
        part = dot_nn(rows_vmem[:, n * half : (n + 1) * half], c_vmem[n * half : (n + 1) * half, :])
        acc = part if acc is None else acc + part
    copies[4].wait()
    acc = acc + sum_ref[...]
    cols = []
    for s in range(2):
        gate = acc[:, 256 * s : 256 * s + 128]
        up = acc[:, 256 * s + 128 : 256 * s + 256]
        cols.append((gate / (1.0 + jnp.exp(-gate)) * up).astype(BF))
    res = jnp.concatenate(cols, axis=1)
    res_ref[pl.ds(pl.multiple_of(core * caps, caps), caps), :] = res[:caps]
    res_ref[pl.ds(pl.multiple_of((1 - core) * caps, caps), caps), :] = res[caps:]
    copies = [pltpu.make_async_copy(res_ref, out_ref.at[g], out_sems.at[g]) for g in range(4)]
    for copy in copies:
        copy.start()
    for copy in copies:
        copy.wait()


def down_body(ord_ref, idx_ref, first_ref, second_ref, hid_ref, mate_ref, out_ref, scr, w_ref, sems):
    caps = idx_ref.shape[1]
    rows, unit, acc = 512, 24, None
    copies = [
        pltpu.make_async_copy(r, w_ref.at[pl.ds(192 * n, 192)], sems.at[n]) for n, r in enumerate((first_ref, second_ref))
    ]
    for copy in copies:
        copy.start()
    for copy in copies:
        copy.wait()
    for core, h_ref in ((ord_ref[32], hid_ref), (1 - ord_ref[32], mate_ref)):
        for x in range(4):
            lo = pl.multiple_of(512 * x + 256 * core, 256)
            part = dot_nt(w_ref[:, pl.ds(lo, 256)], h_ref[x])
            acc = part if acc is None else acc + part
    for k in range(16):
        at = pl.multiple_of(ord_ref[16 + k] * unit, 8)
        scr[pl.ds(at, unit), :] = acc[k * unit : (k + 1) * unit, :]
    for b in range(2):
        hot = (lax.broadcasted_iota(jnp.int32, (rows, caps), 0) == idx_ref[b : b + 1, :]).astype(BF)
        dense = dot_nt(hot, scr[:, b * caps : (b + 1) * caps].astype(BF)).astype(BF)
        for n in range(16):
            out_ref[16 * b + n] = dense[32 * n : 32 * n + 32, :]


def spread_body(*refs):
    out_ref, sems = refs[-2], refs[-1]
    lo, copies = 0, []
    for n, r in enumerate(refs[:-2]):
        for q in range(out_ref.shape[0]):
            copies.append(pltpu.make_async_copy(r, out_ref.at[q, pl.ds(lo, r.shape[0])], sems.at[n, q]))
        lo += r.shape[0]
    for copy in copies:
        copy.start()
    for copy in copies:
        copy.wait()


def quarter_body(in_ref, out_ref):
    for x in range(4):
        out_ref[:, 512 * x : 512 * (x + 1)] = in_ref[24 * x : 24 * (x + 1), :]


def place_body(in_ref, scale_ref, out_ref, scr):
    unit = 24
    for g in range(8):
        core, x = g // 4, g % 4
        acc = in_ref[16 * core + x].astype(F32)
        for q in range(1, 4):
            acc = acc + in_ref[16 * core + 4 * q + x].astype(F32)
        turned = acc.T
        for m in range(16):
            lo = 192 * m + 96 * core + unit * x
            scr[lo : lo + unit, :] = turned[m * unit : (m + 1) * unit, :]
    for n in range(6):
        out_ref[:, n * 512 : (n + 1) * 512] = (scr[n * 512 : (n + 1) * 512, :].T * scale_ref[...]).astype(BF)


def pairs(step):
    flips = ((1, 3), (3, 1))
    return [(2 * i + c, 2 * (i ^ flips[c][step]) + c) for i in range(4) for c in range(2)]


def join_body(a_ref, b_ref, out_ref):
    rows = a_ref.shape[0]
    out_ref[:rows, :] = a_ref[...]
    out_ref[rows:, :] = b_ref[...]


def join(a, b):
    out = jax.ShapeDtypeStruct((a.shape[0] + b.shape[0], a.shape[1]), BF)
    return call(join_body, out, [vm(), vm()], mib=4)(a, b)


def meet(value, axis, step):
    return lax.ppermute(value, (axis, "c"), pairs(step))


def over_y(parts):
    rows, cols = sum(p.shape[0] for p in parts), parts[0].shape[1]
    wide = call(
        spread_body,
        pltpu.HBM((4, rows, cols), BF),
        [vm()] * len(parts),
        scratch=[pltpu.SemaphoreType.DMA((len(parts), 4))],
        mib=4,
        to=hb,
    )(*parts)
    return lax.all_to_all(wide, "y", 0, 0, tiled=True)


def near_y(value):
    near = meet(value, "y", 0)
    other = meet(value, "y", 1)
    return value, near, other, meet(near, "y", 1)


def shards(tokens, expert_ids, route_weight, index_list, gate_weight, up_weight, down_weight):
    zh, y, c, zl, x = (lax.axis_index(n) for n in ("zh", "y", "c", "zl", "x"))
    caps = index_list.shape[1]

    cut = lambda w, n: w[:, 128 * n : 128 * n + 128]
    mine = [
        jnp.concatenate([cut(w, 2 * h + s) for s in range(2) for w in (gate_weight, up_weight)], axis=1)
        for h in range(2)
    ]
    both_rows = lax.all_to_all(jnp.concatenate(mine, axis=0), "c", 0, 0, tiled=True)

    turned = down_weight.T
    quarter = lax.all_to_all(turned, "x", 0, 0, tiled=True)
    quarter = call(quarter_body, jax.ShapeDtypeStruct((24, 2048), BF), [vm()], mib=4)(quarter)

    flip = jnp.where(c == 0, jnp.array([0, 1, 3, 2]), jnp.array([0, 3, 1, 2])).astype(jnp.int32)
    order = ((zh ^ flip)[None, :] * 4 + jnp.arange(4, dtype=jnp.int32)[:, None]).reshape(16)
    order_down = ((zh ^ flip)[None, :] * 4 + (y ^ flip)[:, None]).reshape(16)
    order = jnp.concatenate([order, order_down, c.reshape(1)]).astype(jnp.int32)

    rows = call(
        pick_body, jax.ShapeDtypeStruct((16, caps, 256), BF), [vm(), vm()], flops=2 * 256 * 512 * 3072
    )(index_list.reshape(caps, 1), tokens)
    swap = [(0, 1), (1, 0)]
    rows_mate = lax.ppermute(rows, "c", swap)
    index_mate = lax.ppermute(index_list, "c", swap)
    index_both = jnp.where(
        c == 0,
        jnp.concatenate([index_list, index_mate], axis=0),
        jnp.concatenate([index_mate, index_list], axis=0),
    )

    near = meet(both_rows, "zh", 0)
    both = join(both_rows, near)
    far = meet(both, "zh", 1)
    soon = near_y(both)
    yc = over_y((far,))

    near = meet(quarter, "zh", 0)
    two = join(quarter, near)
    far = pltpu.with_memory_space_constraint(meet(two, "zh", 1), pltpu.HBM)
    four = join(two, far)
    near = pltpu.with_memory_space_constraint(meet(four, "y", 0), pltpu.HBM)
    down_first = join(four, near)
    down_second = meet(down_first, "y", 1)

    yc = yc.reshape(1536, 512)
    early, rows_late = call(
        early_body,
        [pltpu.HBM((512, 512), F32), pltpu.HBM((512, 1536), BF)],
        [sm()] + [vm()] * 6,
        scratch=[pltpu.VMEM((512, 1536), BF)] * 2 + [pltpu.VMEM((512, 512), F32), pltpu.SemaphoreType.DMA((2,))],
        flops=512 * 3072 * 512,
        to=hb,
    )(order, rows, rows_mate, *soon)
    early, rows_late = (pltpu.with_memory_space_constraint(v, pltpu.HBM) for v in (early, rows_late))
    wide = call(
        hidden_body,
        pltpu.HBM((4, 512, 256), BF),
        [sm(), hb(), hb(), hb()],
        scratch=[
            pltpu.VMEM((512, 256), BF),
            pltpu.VMEM((512, 1536), BF),
            pltpu.VMEM((1536, 512), BF),
            pltpu.VMEM((512, 512), F32),
            pltpu.SemaphoreType.DMA((5,)),
            pltpu.SemaphoreType.DMA((4,)),
        ],
        flops=512 * 3072 * 512,
        to=hb,
    )(order, rows_late, early, yc)
    hid = lax.all_to_all(wide, "x", 0, 0, tiled=True)
    hid_mate = lax.ppermute(hid, "c", swap)

    parts = call(
        down_body,
        jax.ShapeDtypeStruct((32, 32, 384), BF),
        [sm(), vm(), hb(), hb(), vm(), vm()],
        scratch=[pltpu.VMEM((384, 512), F32), pltpu.VMEM((384, 2048), BF), pltpu.SemaphoreType.DMA((2,))],
        flops=2 * 512 * 384 * 2048,
    )(order, index_both, down_first, down_second, hid, hid_mate)
    owned = lax.all_to_all(parts, ("c", "zl", "x"), 0, 0, tiled=True)

    start = (zl * 4 + x) * 32
    ids = lax.dynamic_slice_in_dim(expert_ids, start, 32, 0)
    weights = lax.dynamic_slice_in_dim(route_weight, start, 32, 0)
    scale = jnp.sum(jnp.where(ids == 0, weights, jnp.zeros_like(weights)), axis=1, keepdims=True)
    return call(
        place_body, jax.ShapeDtypeStruct((32, 3072), BF), [vm(), vm()], mib=8, scratch=[pltpu.VMEM((3072, 32), F32)]
    )(owned, scale)


def solution(mesh):
    fine = Mesh(mesh.devices.reshape(4, 4, 2, 4, 4), ("zh", "y", "c", "zl", "x"))
    edp, etp = ("zh", "y", "c"), ("zl", "x")
    in_specs = (P(edp, None), P(edp, None), P(edp, None), P(edp, None), P(edp, etp), P(edp, etp), P(etp, edp))

    return jax.shard_map(shards, mesh=fine, in_specs=in_specs, out_specs=P(edp + etp, None), check_vma=False)
```
